256 devices in a mesh: dp: 8 (over z_hi, x), ha: 4 (over y), wa: 8 (over z_lo, core).
Axes of the slice: x: 4, y: 4, z: 8 (z_hi: 2, z_lo: 4; z = z_hi * 4 + z_lo), core: 2. Of those that a mesh axis runs over, the one named last changes fastest.
Arguments:
- queries: bfloat16 [8, 1, 4, 8, 144, 768], P('dp', None, 'ha', 'wa'), may hold values from -5 to 5
- key_tiles: bfloat16 [8, 1, 4, 8, 144, 768], P('dp', None, 'ha', 'wa'), may hold values from -5 to 5
- value_tiles: bfloat16 [8, 1, 4, 8, 144, 768], P('dp', None, 'ha', 'wa'), may hold values from -6 to 6
- out_grad: bfloat16 [8, 1, 4, 8, 144, 1536], P('dp', None, 'ha', 'wa'), may hold values from -8 to 8
- w_out: bfloat16 [1536, 768], replicated, may hold values from -0.21875 to 0.21875
- reaches: int32 [6, 6], replicated, may hold values from 0 to 1, as said below
Outputs:
- grad_query: bfloat16 [8, 1, 4, 8, 144, 768], P('dp', None, 'ha', 'wa')
- grad_key: bfloat16 [8, 1, 4, 8, 144, 768], P('dp', None, 'ha', 'wa')
- grad_value: bfloat16 [8, 1, 4, 8, 144, 768], P('dp', None, 'ha', 'wa')
- grad_w_out: float32 [1536, 768], P(('dp', 'ha', 'wa'))
The draws below stay inside these ranges and needn't reach their ends.
Inputs may be any that keep to these rules, and one draw needn't show every extreme that they name: `reaches`: some head has every entry 1, and some other head has every entry 0.
All inputs are finite; a program needn't handle non-finite values.
Results may differ from the reference program's by a relative error of at most 0.018.
Values may be sent and summed in bfloat16 or wider, within the bound.
A program may use at most 128 MiB of HBM per device.

```python
import math
import jax
import jax.numpy as jnp
from jax import lax

D = 1536
HEADS = 6
HD = 128
NT = 1
TILE = 144
HQ = 768
B = 8
NH = 4
NW = 8


def draw_queries(key, part):
    shape_rows = (B * NT * NH * NW * TILE, HQ)
    own_key = jax.random.fold_in(key, 11)
    flat_rows = jax.random.truncated_normal(own_key, -4.0, 4.0, shape_rows, jnp.float32)
    return flat_rows.reshape(B, NT, NH, NW, TILE, HQ).astype(jnp.bfloat16)


def draw_key_tiles(key, part):
    shape_rows = (B * NT * NH * NW * TILE, HQ)
    own_key = jax.random.fold_in(key, 12)
    flat_rows = jax.random.truncated_normal(own_key, -4.0, 4.0, shape_rows, jnp.float32)
    return flat_rows.reshape(B, NT, NH, NW, TILE, HQ).astype(jnp.bfloat16)


def draw_reaches(key, part):
    first_head = jax.random.randint(jax.random.fold_in(key, 21), (), 0, HEADS)
    second_head = (first_head + 1 + jax.random.randint(jax.random.fold_in(key, 22), (), 0, HEADS - 1)) % HEADS
    random_bits = jax.random.randint(jax.random.fold_in(key, 23), (HEADS, 6), 0, 2)
    head_ids = jnp.arange(HEADS)[:, None]
    chosen = jnp.where(head_ids == first_head, 1, jnp.where(head_ids == second_head, 0, random_bits))
    return chosen.astype(jnp.int32)


def spiked(result, key, source, target, blocks, factor):
    def block_of(position):
        return (jnp.arange(result.shape[position]) // (result.shape[position] // blocks)).reshape((-1,) + (1,) * (result.ndim - 1 - position))

    one_side = jax.random.permutation(key, blocks)[block_of(target)]
    other_side = (block_of(target) + blocks // 2) % blocks
    return jnp.where((block_of(source) == one_side) | (block_of(source) == other_side), factor * result, result)


def steps_of(stream_key, shape, shards, least, top_value):
    loudness = 1.0
    for axis_at, shards_of in shards:
        heights = jax.random.uniform(jax.random.fold_in(jax.random.fold_in(stream_key, 6), axis_at), (shards_of,), jnp.float32, least / len(shards), top_value / len(shards))
        loudness = loudness * jnp.repeat(jnp.exp(heights), shape[axis_at] // shards_of).reshape((-1,) + (1,) * (len(shape) - 1 - axis_at))
    return loudness


def gaussian(key, extent, deviation, limit, shards=(), kind=jnp.bfloat16):
    result = jax.random.normal(key, extent, jnp.float32) * deviation
    if len(shards) > 0:
        result = steps_of(key, extent, shards, -0.22, 0.18) * result
    return jnp.clip(result, min=-limit, max=limit).astype(kind)


def gaussian_with(rng, extent, spread, most, cuts, heavy, dtype=jnp.bfloat16):
    result = spread * jax.random.normal(rng, extent, jnp.float32)
    if cuts:
        result = result * steps_of(rng, extent, cuts, -0.22, 0.18)
    return jnp.clip(spiked(result, jax.random.fold_in(rng, 3), *heavy), -most, most).astype(dtype)


def setup_inputs(seed: int = 0) -> dict:
    arg_keys = jax.random.split(jax.random.key(seed), 7)
    return {
        "queries": draw_queries(jax.random.fold_in(arg_keys[6], 71), 0),
        "key_tiles": draw_key_tiles(jax.random.fold_in(arg_keys[6], 71), 0),
        "value_tiles": gaussian(arg_keys[2], (B, NT, NH, NW, TILE, HQ), 1.0, 6.0, ((0, 8), (2, 4), (3, 8))),
        "out_grad": gaussian_with(arg_keys[3], (B, NT, NH, NW, TILE, D), 1.0, 8.0, ((0, 8), (2, 4), (3, 8)), (3, 5, 8, 2.0)),
        "w_out": gaussian(arg_keys[4], (D, HQ), HQ ** -0.5, 0.21875),
        "reaches": draw_reaches(jax.random.fold_in(arg_keys[6], 71), 0),
    }


def neighbours(tile_field):
    padded = jnp.pad(tile_field, ((0, 0), (1, 1), (1, 1), (0, 0), (0, 0)))
    stacked = jnp.stack([jnp.stack([padded[:, row_off:row_off + NH, col_off:col_off + NW] for col_off in range(3)], 0) for row_off in range(3)], 0)
    arranged = jnp.transpose(stacked, (3, 4, 2, 0, 1, 5, 6))
    return arranged.reshape(NH, NW, NT * 9 * TILE, tile_field.shape[-1])

def fold_back(contrib):
    channels = contrib.shape[-1]
    pieces = contrib.reshape(NH, NW, NT, 3, 3, TILE, channels)
    summed = jnp.zeros((NT, NH + 2, NW + 2, TILE, channels), jnp.float32)
    for row_off in range(3):
        for col_off in range(3):
            summed = summed.at[:, row_off:row_off + NH, col_off:col_off + NW].add(jnp.transpose(pieces[:, :, :, row_off, col_off], (2, 0, 1, 3, 4)))
    return summed[:, 1:NH + 1, 1:NW + 1]

def allowed_pairs(reach_row):
    time_ids = jnp.arange(NT)
    t_delta = time_ids[None, :] - time_ids[:, None]
    time_ok = (t_delta >= -reach_row[0]) & (t_delta <= reach_row[1])
    offsets = jnp.arange(3) - 1
    row_pos = jnp.arange(NH)[:, None] + offsets[None, :]
    row_ok = ((offsets >= -reach_row[2]) & (offsets <= reach_row[3]))[None, :] & (row_pos >= 0) & (row_pos < NH)
    col_pos = jnp.arange(NW)[:, None] + offsets[None, :]
    col_ok = ((offsets >= -reach_row[4]) & (offsets <= reach_row[5]))[None, :] & (col_pos >= 0) & (col_pos < NW)
    tile_pairs = time_ok[None, None, :, :, None, None] & row_ok[:, None, None, None, :, None] & col_ok[None, :, None, None, None, :]
    expanded = jnp.broadcast_to(tile_pairs[:, :, :, None, :, :, :, None], (NH, NW, NT, TILE, NT, 3, 3, TILE))
    return expanded.reshape(NH, NW, NT * TILE, NT * 9 * TILE)

def to_columns(tile_field):
    return jnp.transpose(tile_field, (1, 2, 0, 3, 4)).reshape(NH, NW, NT * TILE, tile_field.shape[-1])

def from_columns(column_field):
    return jnp.transpose(column_field.reshape(NH, NW, NT, TILE, column_field.shape[-1]), (2, 0, 1, 3, 4))

def sample_grads(inputs, w_out, reaches):
    query_part, key_part, value_part, grad_part = inputs
    softmax_scale = 1.0 / math.sqrt(HD)
    grad_rows = grad_part.astype(jnp.float32).reshape(-1, D)
    grad_attn = jnp.dot(grad_rows, w_out.astype(jnp.float32)).astype(jnp.bfloat16).reshape(NT, NH, NW, TILE, HQ)
    attn_list, gq_list, gk_list, gv_list = ([], [], [], [])
    for head_index in range(HEADS):
        col_start = head_index * HD
        col_stop = col_start + HD
        query_head = to_columns(query_part[..., col_start:col_stop].astype(jnp.float32))
        grad_head = to_columns(grad_attn[..., col_start:col_stop].astype(jnp.float32))
        key_near = neighbours(key_part[..., col_start:col_stop].astype(jnp.float32))
        value_near = neighbours(value_part[..., col_start:col_stop].astype(jnp.float32))
        allowed = allowed_pairs(reaches[head_index])
        scores = jnp.einsum('ijad,ijbd->ijab', query_head, key_near) * softmax_scale
        masked = jnp.where(allowed, scores, -jnp.inf)
        row_peak = lax.optimization_barrier(jnp.max(masked, axis=-1, keepdims=True))
        exp_terms = jnp.exp(masked - row_peak)
        prob_rows = exp_terms / lax.optimization_barrier(jnp.sum(exp_terms, axis=-1, keepdims=True))
        probs_wide = lax.optimization_barrier(prob_rows.astype(jnp.bfloat16)).astype(jnp.float32)
        attn_head = jnp.einsum('ijab,ijbd->ijad', probs_wide, value_near).astype(jnp.bfloat16)
        row_delta = lax.optimization_barrier(jnp.sum(grad_head * attn_head.astype(jnp.float32), axis=-1, keepdims=True))
        grad_probs = jnp.einsum('ijad,ijbd->ijab', grad_head, value_near)
        grad_scores = lax.optimization_barrier((prob_rows * (grad_probs - row_delta)).astype(jnp.bfloat16)).astype(jnp.float32)
        grad_q_head = (jnp.einsum('ijab,ijbd->ijad', grad_scores, key_near) * softmax_scale).astype(jnp.bfloat16)
        grad_k_near = jnp.einsum('ijab,ijad->ijbd', grad_scores, query_head) * softmax_scale
        grad_v_near = jnp.einsum('ijab,ijad->ijbd', probs_wide, grad_head)
        attn_list.append(from_columns(attn_head))
        gq_list.append(from_columns(grad_q_head))
        gk_list.append(fold_back(grad_k_near))
        gv_list.append(fold_back(grad_v_near))
    attended = jnp.concatenate(attn_list, axis=-1)
    grad_q = jnp.concatenate(gq_list, axis=-1)
    grad_k = jnp.concatenate(gk_list, axis=-1).astype(jnp.bfloat16)
    grad_v = jnp.concatenate(gv_list, axis=-1).astype(jnp.bfloat16)
    grad_w = jnp.dot(grad_rows.T, attended.astype(jnp.float32).reshape(-1, HQ))
    return (grad_q, grad_k, grad_v, grad_w)

def reference(queries, key_tiles, value_tiles, out_grad, w_out, reaches):

    def per_sample(inputs):
        return sample_grads(inputs, w_out, reaches)
    grad_q, grad_k, grad_v, grad_w = lax.map(per_sample, (queries, key_tiles, value_tiles, out_grad))
    return (grad_q, grad_k, grad_v, lax.optimization_barrier(jnp.sum(grad_w, axis=0)))
```

```python
import math

import jax
import jax.numpy as jnp
from jax import lax
from jax.experimental import pallas as pl
from jax.experimental.pallas import tpu as pltpu
from jax.sharding import PartitionSpec as P

MESH = pl.DeviceIdType.MESH
HEADS = 6
HALO = 5
HD = 128
TILE = 144
KEYS = 9 * TILE
HQ = HEADS * HD
D = 1536
SCALE = 1.0 / math.sqrt(HD)
ROWS = 16
BF = jnp.bfloat16
F32 = jnp.float32
ANY_COLS = (0, 2)


def dot(a, b):
    return jnp.dot(a, b, preferred_element_type=F32)


def dot_nt(a, b):
    return lax.dot_general(a, b, (((1,), (1,)), ((), ())), preferred_element_type=F32)


def kernel(
    reach, q_in, k_in, v_in, og_in, w_in,
    gq_out, gk_out, gv_out, gw_out,
    q_v, k_v, v_v, og_v, w_v, a_v, ogt, kv, qa, kv0, qa0, stat, sb, trow,
    s_buf, dp_buf, p_buf, ds_buf, att_buf, res,
    gbuf, rbuf, abuf, x1buf, xs, x2buf, cbuf, ybuf, zbuf, zr, fbuf, f2, gws,
    in_sem, yk_s, yk_r, yq_s, yq_r, wk_s, wk_r, wq_s, wq_r, sy_s, sy_r, sw_s, sw_r,
    dd_s, dd_r, x1_s, x1_r, x2_s, x2_r, yy_s, yy_r, zz_s, zz_r, fin_s, fin_r,
):
    dp = lax.axis_index("dp")
    ha = lax.axis_index("ha")
    wa = lax.axis_index("wa")
    x = lax.rem(dp, 4)
    z_hi = lax.div(dp, 4)
    core = lax.rem(wa, 2)
    z_lo = lax.div(wa, 2)
    zi = z_hi * 4 + z_lo
    mate = wa + 1 - 2 * core
    x_one = x + 1 - 2 * lax.rem(x, 2)
    x_three = 3 - x
    x_far = lax.rem(x + 2, 4)
    x_a = x_one + core * (x_three - x_one)
    x_b = x_three + core * (x_one - x_three)
    has_left = wa > 0
    has_right = wa < 7

    def at(dp_=dp, ha_=ha, wa_=wa):
        return (dp_, ha_, wa_)

    barrier = pltpu.get_barrier_semaphore()

    def greet(device):
        pl.semaphore_signal(barrier, inc=1, device_id=device, device_id_type=MESH)

    for dy in (1, 2, 3):
        greet(at(ha_=lax.rem(ha + dy, 4)))
    greet(at(wa_=mate))
    greet(at(dp_=z_hi * 4 + x_one))
    greet(at(dp_=z_hi * 4 + x_three))

    def z_device(dz):
        zt = lax.rem(zi + dz, 8)
        return at(dp_=lax.div(zt, 4) * 4 + x, wa_=lax.rem(zt, 4) * 2 + core)

    for dz in range(1, 8):
        greet(z_device(dz))
    far_right = (core == 1) & has_right
    far_left = (core == 0) & has_left

    @pl.when(far_right)
    def _():
        greet(at(wa_=wa + 1))

    @pl.when(far_left)
    def _():
        greet(at(wa_=wa - 1))

    loads = [
        pltpu.make_async_copy(src, dst, in_sem.at[n])
        for n, (src, dst) in enumerate(
            ((k_in, k_v), (v_in, v_v), (q_in, q_v), (og_in, og_v), (w_in, w_v))
        )
    ]
    for load in loads:
        load.start()

    zero_head = jnp.int32(0)
    for n in reversed(range(HEADS)):
        total = reach[n, 0]
        for t in range(1, 6):
            total = total + reach[n, t]
        zero_head = jnp.where(total == 0, n, zero_head)

    def columns(ref, head):
        return ref[:, head * HD : (head + 1) * HD]

    def slot_columns(ref, slot):
        return jnp.where(slot >= zero_head, columns(ref, slot + 1), columns(ref, slot))

    def zero_columns(ref):
        value = columns(ref, 0)
        for h in range(1, HEADS):
            value = jnp.where(zero_head == h, columns(ref, h), value)
        return value

    def head_value(of_slot, h):
        value = jnp.where(zero_head == h, of_slot(HALO), of_slot(min(h, HALO - 1)))
        return jnp.where(zero_head < h, of_slot(h - 1), value) if h else value

    @pl.when(wa == 0)
    def _():
        for buf in (kv, qa):
            def clear(s, carry, buf=buf):
                for kind in range(2):
                    for r in range(3):
                        buf[s, kind, r, 0] = jnp.zeros((TILE, HD), BF)
                return carry
            lax.fori_loop(0, HALO, clear, 0)
        for r in range(3):
            sb[r, 0] = jnp.zeros((TILE, HD), BF)

    @pl.when(wa == 7)
    def _():
        for buf in (kv, qa):
            def clear(s, carry, buf=buf):
                for kind in range(2):
                    for r in range(3):
                        buf[s, kind, r, 2] = jnp.zeros((TILE, HD), BF)
                return carry
            lax.fori_loop(0, HALO, clear, 0)
        for r in range(3):
            sb[r, 2] = jnp.zeros((TILE, HD), BF)

    loads[0].wait()
    loads[1].wait()

    for s in range(HALO):
        kv[s, 0, 1, 1] = slot_columns(k_v, s)
        kv[s, 1, 1, 1] = slot_columns(v_v, s)
    kv0[0] = zero_columns(k_v)
    kv0[1] = zero_columns(v_v)

    ha_up = lax.rem(ha + 3, 4)
    ha_down = lax.rem(ha + 1, 4)
    wa_right = jnp.minimum(wa + 1, 7)
    wa_left = jnp.maximum(wa - 1, 0)

    def y_copy(buf, send, recv, s, r):
        return pltpu.make_async_remote_copy(
            src_ref=buf.at[s, :, 1, 1], dst_ref=buf.at[s, :, r, 1],
            send_sem=send.at[s, r // 2], recv_sem=recv.at[s, r // 2],
            device_id=at(ha_=ha_up if r == 2 else ha_down), device_id_type=MESH,
        )

    def w_copy(buf, send, recv, s, r, c):
        return pltpu.make_async_remote_copy(
            src_ref=buf.at[s, :, r, 1], dst_ref=buf.at[s, :, r, c],
            send_sem=send.at[s, r, c // 2], recv_sem=recv.at[s, r, c // 2],
            device_id=at(wa_=wa_right if c == 0 else wa_left), device_id_type=MESH,
        )

    sends_to = {0: has_right, 2: has_left}
    gets_from = {0: has_left, 2: has_right}

    def w_send(buf, send, recv, s, r):
        for c in ANY_COLS:
            @pl.when(sends_to[c])
            def _(c=c):
                w_copy(buf, send, recv, s, r, c).start()

    def relay(buf, y_send, y_recv, w_s, w_r, s):
        for r in (0, 2):
            y_copy(buf, y_send, y_recv, s, r).wait_recv()
            w_send(buf, w_s, w_r, s, r)

    def w_wait(buf, send, recv, s):
        for c in ANY_COLS:
            @pl.when(gets_from[c])
            def _(c=c):
                for r in range(3):
                    w_copy(buf, send, recv, s, r, c).wait_recv()

    def relay_kv(s):
        relay(kv, yk_s, yk_r, wk_s, wk_r, s)

    def relay_qa(s):
        relay(qa, yq_s, yq_r, wq_s, wq_r, s)

    pl.semaphore_wait(barrier, 13 + (far_right | far_left).astype(jnp.int32))

    def first_kv(s, carry):
        for r in (0, 2):
            y_copy(kv, yk_s, yk_r, s, r).start()
        w_send(kv, wk_s, wk_r, s, 1)
        return carry

    lax.fori_loop(0, HALO, first_kv, 0)

    loads[2].wait()
    loads[3].wait()
    loads[4].wait()
    a_v[...] = dot(og_v[...], w_v[...]).astype(BF)

    for s in range(HALO):
        qa[s, 0, 1, 1] = slot_columns(q_v, s)
        qa[s, 1, 1, 1] = slot_columns(a_v, s)
        for r in (0, 2):
            y_copy(qa, yq_s, yq_r, s, r).start()
    qa0[0] = zero_columns(q_v)
    qa0[1] = zero_columns(a_v)

    eye = (
        lax.broadcasted_iota(jnp.int32, (HD, HD), 0) == lax.broadcasted_iota(jnp.int32, (HD, HD), 1)
    ).astype(F32).astype(BF)
    for t in range(D // HD):
        ogt[t * HD : (t + 1) * HD, :] = dot_nt(eye, og_v[:, t * HD : (t + 1) * HD]).astype(BF)

    stat[...] = jnp.zeros((TILE, HD), F32)
    lane = lax.broadcasted_iota(jnp.int32, (ROWS, HD), 1)
    key_id = lax.broadcasted_iota(jnp.int32, (1, KEYS), 1)
    place = jnp.zeros((1, KEYS), jnp.int32)
    for n in range(1, 9):
        place = place + (key_id >= n * TILE).astype(jnp.int32)
    row_id = (key_id >= 3 * TILE).astype(jnp.int32) + (key_id >= 6 * TILE).astype(jnp.int32)
    col_id = place - 3 * row_id

    def bias_row(s, mirrored):
        later = s >= zero_head
        up, down, left, right = (jnp.where(later, reach[s + 1, t], reach[s, t]) for t in range(2, 6))
        if mirrored:
            up, down, left, right = down, up, right, left

        def bias(ok):
            return jnp.where(ok, 0.0, -jnp.inf).astype(F32)

        b_up = bias((up > 0) & (ha > 0))
        b_down = bias((down > 0) & (ha < 3))
        b_left = bias((left > 0) & has_left)
        b_right = bias((right > 0) & has_right)
        zero = jnp.zeros((1, KEYS), F32)
        by_row = jnp.where(row_id == 0, zero + b_up, jnp.where(row_id == 2, zero + b_down, zero))
        by_col = jnp.where(col_id == 0, zero + b_left, jnp.where(col_id == 2, zero + b_right, zero))
        return by_row + by_col

    def split3(value):
        high = value.astype(BF).astype(F32)
        rest = value - high
        mid = rest.astype(BF).astype(F32)
        return high, mid, rest - mid

    def forward(slot, q, a, k, v, bias):
        n = k.shape[0]
        s_buf[:, :n] = dot_nt(q, k)
        dp_buf[:, :n] = dot_nt(a, v)

        def rows_step(i, carry):
            rows = pl.ds(pl.multiple_of(i * ROWS, ROWS), ROWS)
            s = s_buf[rows, :n] * SCALE
            if bias is not None:
                s = s + bias
            d = dp_buf[rows, :n]
            peak = jnp.max(s, axis=1, keepdims=True)
            e = jnp.exp(s - peak)
            total = jnp.sum(e, axis=1, keepdims=True)
            p = e * (1.0 / total)
            delta = jnp.sum(p * d, axis=1, keepdims=True)
            p_buf[rows, :n] = p.astype(BF)
            ds_buf[rows, :n] = (p * (d - delta)).astype(BF)
            block = stat[rows, :]
            for base, parts in ((0, split3(peak + jnp.log(total))), (64, split3(delta))):
                for t, part in enumerate(parts):
                    block = jnp.where(lane == base + 3 * slot + t, part, block)
            stat[rows, :] = block
            return carry

        lax.fori_loop(0, TILE // ROWS, rows_step, 0)
        att_buf[...] = dot(p_buf[:, :n], v).astype(BF)
        res[0, slot] = (dot(ds_buf[:, :n], k) * SCALE).astype(BF)

    def backward(slot, k, v, q, a, lse_row, delta_row):
        n = q.shape[0]
        s_buf[:, :n] = dot_nt(k, q)
        dp_buf[:, :n] = dot_nt(v, a)

        def rows_step(i, carry):
            rows = pl.ds(pl.multiple_of(i * ROWS, ROWS), ROWS)
            p = jnp.exp(s_buf[rows, :n] * SCALE - lse_row)
            p_buf[rows, :n] = p.astype(BF)
            ds_buf[rows, :n] = (p * (dp_buf[rows, :n] - delta_row)).astype(BF)
            return carry

        lax.fori_loop(0, TILE // ROWS, rows_step, 0)
        res[2, slot] = dot(p_buf[:, :n], a).astype(BF)
        res[1, slot] = (dot(ds_buf[:, :n], q) * SCALE).astype(BF)

    def weight_term(index):
        def step(t, carry):
            rows = pl.ds(pl.multiple_of(t * 192, 192), 192)
            gbuf[index, lax.div(t, 4), lax.rem(t, 4)] = dot(ogt[rows, :], att_buf[...]).astype(BF)
            return carry

        lax.fori_loop(0, 8, step, 0)

    def mate_copy(j):
        return pltpu.make_async_remote_copy(
            src_ref=gbuf.at[2 * j + 1 - core], dst_ref=rbuf.at[j],
            send_sem=dd_s.at[j], recv_sem=dd_r.at[j], device_id=at(wa_=mate), device_id_type=MESH,
        )

    def x1_copy(j, which):
        return pltpu.make_async_remote_copy(
            src_ref=abuf.at[j, :, x_far if which else x_a], dst_ref=x1buf.at[j, which],
            send_sem=x1_s.at[j, which], recv_sem=x1_r.at[j, which],
            device_id=at(dp_=z_hi * 4 + x_a), device_id_type=MESH,
        )

    def x2_copy(j):
        return pltpu.make_async_remote_copy(
            src_ref=xs.at[j], dst_ref=x2buf.at[j],
            send_sem=x2_s.at[j], recv_sem=x2_r.at[j],
            device_id=at(dp_=z_hi * 4 + x_b), device_id_type=MESH,
        )

    def y_sum_copy(dy):
        to = lax.rem(ha + dy, 4)
        return pltpu.make_async_remote_copy(
            src_ref=cbuf.at[:, :, to], dst_ref=ybuf.at[dy - 1],
            send_sem=yy_s.at[dy - 1], recv_sem=yy_r.at[dy - 1],
            device_id=at(ha_=to), device_id_type=MESH,
        )

    def z_sum_copy(dz):
        return pltpu.make_async_remote_copy(
            src_ref=zbuf.at[:, lax.rem(zi + dz, 8)], dst_ref=zr.at[dz - 1],
            send_sem=zz_s.at[dz - 1], recv_sem=zz_r.at[dz - 1],
            device_id=z_device(dz), device_id_type=MESH,
        )

    def last_copy():
        return pltpu.make_async_remote_copy(
            src_ref=fbuf.at[:, 1 - core], dst_ref=f2, send_sem=fin_s.at[0], recv_sem=fin_r.at[0],
            device_id=at(wa_=mate), device_id_type=MESH,
        )

    def wide(value):
        return value.astype(F32)

    def add_mate(j):
        mate_copy(j).wait_recv()

        def add(at_x):
            for h in range(2):
                abuf[j, h, at_x] = (
                    wide(gbuf[2 * j + core, h, at_x]) + wide(rbuf[j, h, at_x])
                ).astype(BF)

        add(x_far)
        x1_copy(j, 1).start()
        add(x_a)
        x1_copy(j, 0).start()
        add(x_b)
        add(x)

    def add_x1(j):
        x1_copy(j, 1).wait_recv()
        for h in range(2):
            xs[j, h] = (wide(abuf[j, h, x_b]) + wide(x1buf[j, 1, h])).astype(BF)
        x2_copy(j).start()

    def add_x2(j):
        x1_copy(j, 0).wait_recv()
        x2_copy(j).wait_recv()
        for h in range(2):
            total = wide(abuf[j, h, x]) + wide(x1buf[j, 0, h]) + wide(x2buf[j, h])
            cbuf[j, h] = total.astype(BF).reshape(4, 48, HD)

    def send_y():
        for dy in (2, 1, 3):
            y_sum_copy(dy).start()

    pick = (lax.broadcasted_iota(jnp.int32, (128, 96), 0), lax.broadcasted_iota(jnp.int32, (128, 96), 1))

    def add_y():
        spread = (
            ((pick[0] & 7) < 6) & (pick[1] == (pick[0] >> 3) * 6 + (pick[0] & 7))
        ).astype(F32).astype(BF)
        for dy in (1, 2, 3):
            y_sum_copy(dy).wait_recv()
        for j in range(3):
            halves = []
            for h in range(2):
                total = wide(cbuf[j, h, ha])
                for n in range(3):
                    total = total + wide(ybuf[n, j, h])
                halves.append(total.astype(BF))
            rows = dot(spread, jnp.concatenate(halves, axis=0))
            zbuf[j] = rows.astype(BF).reshape(8, 16, HD)
        for dz in (4, 3, 5, 2, 6, 1, 7):
            z_sum_copy(dz).start()

    def add_z():
        for dz in range(1, 8):
            z_sum_copy(dz).wait_recv()
        for j in range(3):
            total = wide(zbuf[j, zi])
            for n in range(7):
                total = total + wide(zr[n, j])
            fbuf[j] = total.reshape(2, 8, HD)
        last_copy().start()

    def finish_weights():
        last_copy().wait_recv()
        for j in range(3):
            gws[2 * j + core] = fbuf[j, core]
            gws[2 * j + 1 - core] = f2[j]
        for h in range(HEADS):
            gw_out[:, h * HD : (h + 1) * HD] = head_value(lambda s: gws[(s + 1) % HEADS, 0:6, :], h)

    forward(HALO, qa0[0], qa0[1], kv0[0], kv0[1], None)
    weight_term(0)
    relay_kv(0)
    relay_kv(1)

    def forward_step(s, carry):
        @pl.when(s < HALO - 2)
        def _():
            relay_kv(s + 2)

        @pl.when(s == HALO - 3)
        def _():
            def own_qa(t, c):
                w_send(qa, wq_s, wq_r, t, 1)
                return c
            lax.fori_loop(0, HALO, own_qa, 0)

        @pl.when(s == 3)
        def _():
            relay_qa(0)
            relay_qa(1)

        @pl.when(s == 4)
        def _():
            relay_qa(2)

        w_wait(kv, wk_s, wk_r, s)
        forward(
            s, qa[s, 0, 1, 1], qa[s, 1, 1, 1],
            kv[s, 0].reshape(KEYS, HD), kv[s, 1].reshape(KEYS, HD), bias_row(s, False),
        )
        weight_term(s + 1)

        @pl.when(lax.rem(s, 2) == 0)
        def _():
            mate_copy(lax.div(s, 2)).start()

        @pl.when(lax.rem(s, 2) == 1)
        def _():
            add_mate(lax.div(s, 2))

        @pl.when((lax.rem(s, 2) == 0) & (s > 0))
        def _():
            add_x1(lax.div(s, 2) - 1)
        return carry

    lax.fori_loop(0, HALO, forward_step, 0)

    sb[1, 1] = stat[...].astype(BF)

    def sy_copy(r):
        return pltpu.make_async_remote_copy(
            src_ref=sb.at[1, 1], dst_ref=sb.at[r, 1], send_sem=sy_s.at[r // 2], recv_sem=sy_r.at[r // 2],
            device_id=at(ha_=ha_up if r == 2 else ha_down), device_id_type=MESH,
        )

    def sw_copy(r, c):
        return pltpu.make_async_remote_copy(
            src_ref=sb.at[r, 1], dst_ref=sb.at[r, c],
            send_sem=sw_s.at[r, c // 2], recv_sem=sw_r.at[r, c // 2],
            device_id=at(wa_=wa_right if c == 0 else wa_left), device_id_type=MESH,
        )

    def sw_send(r):
        for c in ANY_COLS:
            @pl.when(sends_to[c])
            def _(c=c):
                sw_copy(r, c).start()

    for r in (0, 2):
        sy_copy(r).start()
    sw_send(1)
    add_mate(2)
    relay_qa(3)
    relay_qa(4)
    add_x2(0)
    for r in (0, 2):
        sy_copy(r).wait_recv()
        sw_send(r)
    add_x1(2)

    chosen = (lax.broadcasted_iota(jnp.int32, (16, HD), 0), lax.broadcasted_iota(jnp.int32, (16, HD), 1))
    first = (chosen[0] & 7) * 3 + (chosen[0] >> 3) * 64
    take = ((chosen[1] >= first) & (chosen[1] < first + 3) & ((chosen[0] & 7) < 6)).astype(F32).astype(BF)

    own = dot_nt(take, sb[1, 1])
    backward(
        HALO, kv0[0], kv0[1], qa0[0], qa0[1], own[HALO : HALO + 1, :], own[8 + HALO : 9 + HALO, :]
    )
    add_x2(1)
    for c in ANY_COLS:
        @pl.when(gets_from[c])
        def _(c=c):
            for r in range(3):
                sw_copy(r, c).wait_recv()
    trow[...] = dot_nt(take, sb[...].reshape(KEYS, HD))
    add_x2(2)
    send_y()

    def backward_step(s, carry):
        w_wait(qa, wq_s, wq_r, s)
        backward(
            s, kv[s, 0, 1, 1], kv[s, 1, 1, 1], qa[s, 0].reshape(KEYS, HD), qa[s, 1].reshape(KEYS, HD),
            trow[pl.ds(s, 1), :] - bias_row(s, True), trow[pl.ds(s + 8, 1), :],
        )

        @pl.when(s == 0)
        def _():
            add_y()

        @pl.when(s == 2)
        def _():
            add_z()
        return carry

    lax.fori_loop(0, HALO, backward_step, 0)

    for h in range(HEADS):
        cols = slice(h * HD, (h + 1) * HD)
        gq_out[:, cols] = head_value(lambda s: res[0, s], h)
        gk_out[:, cols] = head_value(lambda s: res[1, s], h)
        gv_out[:, cols] = head_value(lambda s: res[2, s], h)
    finish_weights()

    def sent(s, carry):
        for r in (0, 2):
            y_copy(kv, yk_s, yk_r, s, r).wait_send()
            y_copy(qa, yq_s, yq_r, s, r).wait_send()
        for c in ANY_COLS:
            @pl.when(sends_to[c])
            def _(c=c):
                for r in range(3):
                    w_copy(kv, wk_s, wk_r, s, r, c).wait_send()
                    w_copy(qa, wq_s, wq_r, s, r, c).wait_send()
        return carry

    lax.fori_loop(0, HALO, sent, 0)
    for r in (0, 2):
        sy_copy(r).wait_send()
    for c in ANY_COLS:
        @pl.when(sends_to[c])
        def _(c=c):
            for r in range(3):
                sw_copy(r, c).wait_send()
    for j in range(3):
        mate_copy(j).wait_send()
        x1_copy(j, 0).wait_send()
        x1_copy(j, 1).wait_send()
        x2_copy(j).wait_send()
    for dy in (1, 2, 3):
        y_sum_copy(dy).wait_send()
    for dz in range(1, 8):
        z_sum_copy(dz).wait_send()
    last_copy().wait_send()


def shards(queries, key_tiles, value_tiles, out_grad, w_out, reaches):
    dma = pltpu.SemaphoreType.DMA
    vm = pltpu.VMEM
    shapes = [
        vm((TILE, HQ), BF), vm((TILE, HQ), BF), vm((TILE, HQ), BF), vm((TILE, D), BF), vm((D, HQ), BF),
        vm((TILE, HQ), BF), vm((D, TILE), BF),
        vm((HALO, 2, 3, 3, TILE, HD), BF), vm((HALO, 2, 3, 3, TILE, HD), BF),
        vm((2, TILE, HD), BF), vm((2, TILE, HD), BF),
        vm((TILE, HD), F32), vm((3, 3, TILE, HD), BF), vm((16, KEYS), F32),
        vm((TILE, KEYS), F32), vm((TILE, KEYS), F32), vm((TILE, KEYS), BF), vm((TILE, KEYS), BF),
        vm((TILE, HD), BF), vm((3, HEADS, TILE, HD), BF),
        vm((6, 2, 4, 192, HD), BF), vm((3, 2, 4, 192, HD), BF), vm((3, 2, 4, 192, HD), BF),
        vm((3, 2, 2, 192, HD), BF), vm((3, 2, 192, HD), BF), vm((3, 2, 192, HD), BF),
        vm((3, 2, 4, 48, HD), BF), vm((3, 3, 2, 48, HD), BF),
        vm((3, 8, 16, HD), BF), vm((7, 3, 16, HD), BF),
        vm((3, 2, 8, HD), F32), vm((3, 8, HD), F32), vm((6, 8, HD), F32),
        dma((5,)),
    ]
    for extent in ((HALO, 2), (HALO, 2), (HALO, 3, 2), (HALO, 3, 2), (2,), (3, 2), (3,), (3, 2), (3,), (3,), (7,), (1,)):
        shapes += [dma(extent), dma(extent)]
    tile = jax.ShapeDtypeStruct((TILE, HQ), BF)
    anywhere = pl.BlockSpec(memory_space=pl.ANY)
    inside = pl.BlockSpec(memory_space=pltpu.VMEM)
    gq, gk, gv, gw = pl.pallas_call(
        kernel,
        out_shape=(tile, tile, tile, jax.ShapeDtypeStruct((6, HQ), F32)),
        in_specs=[pl.BlockSpec(memory_space=pltpu.SMEM)] + [anywhere] * 5,
        out_specs=(inside,) * 4,
        scratch_shapes=shapes,
        compiler_params=pltpu.CompilerParams(collective_id=0, has_side_effects=True),
    )(
        reaches,
        queries.reshape(TILE, HQ),
        key_tiles.reshape(TILE, HQ),
        value_tiles.reshape(TILE, HQ),
        out_grad.reshape(TILE, D),
        w_out,
    )
    return gq.reshape(queries.shape), gk.reshape(queries.shape), gv.reshape(queries.shape), gw


def solution(mesh):
    tiles = P("dp", None, "ha", "wa", None, None)
    return jax.shard_map(
        shards,
        mesh=mesh,
        in_specs=(tiles, tiles, tiles, tiles, P(), P()),
        out_specs=(tiles, tiles, tiles, P(("dp", "ha", "wa"), None)),
        check_vma=False,
    )
```

```python
import math

import jax
import jax.numpy as jnp
from jax import lax
from jax.experimental import pallas as pl
from jax.experimental.pallas import tpu as pltpu
from jax.sharding import PartitionSpec as P

MESH = pl.DeviceIdType.MESH
HEADS = 6
HALO = 5
HD = 128
TILE = 144
KEYS = 9 * TILE
HQ = HEADS * HD
D = 1536
SCALE = 1.0 / math.sqrt(HD)
ROWS = 16
FORWARD_UNROLL = 9
BF = jnp.bfloat16
F32 = jnp.float32
ANY_COLS = (0, 2)


def dot(a, b):
    return jnp.dot(a, b, preferred_element_type=F32)


def dot_nt(a, b):
    return lax.dot_general(a, b, (((1,), (1,)), ((), ())), preferred_element_type=F32)


def kernel(
    reach_in, q_in, k_in, v_in, og_in, w_in,
    grads_out, gw_out,
    reach, q_v, k_v, v_v, og_v, w_v, a_v, ogt, kv, qa, kv0, qa0, stat, sb, trow,
    s_buf, dp_buf, p_buf, ds_buf, att_buf, res,
    gbuf, rbuf, abuf, x1buf, xs, x2buf, cbuf, ybuf, zbuf, zr, fbuf, f2, gws,
    in_sem, yk_s, yk_r, yq_s, yq_r, wk_s, wk_r, wq_s, wq_r, sy_s, sy_r, sw_s, sw_r,
    dd_s, dd_r, x1_s, x1_r, x2_s, x2_r, yy_s, yy_r, zz_s, zz_r, fin_s, fin_r,
):
    dp = lax.axis_index("dp")
    ha = lax.axis_index("ha")
    wa = lax.axis_index("wa")
    x = lax.rem(dp, 4)
    z_hi = lax.div(dp, 4)
    core = lax.rem(wa, 2)
    z_lo = lax.div(wa, 2)
    zi = z_hi * 4 + z_lo
    mate = wa + 1 - 2 * core
    x_one = x + 1 - 2 * lax.rem(x, 2)
    x_three = 3 - x
    x_far = lax.rem(x + 2, 4)
    x_a = x_one + core * (x_three - x_one)
    x_b = x_three + core * (x_one - x_three)
    has_left = wa > 0
    has_right = wa < 7

    def at(dp_=dp, ha_=ha, wa_=wa):
        return (dp_, ha_, wa_)

    loads = [
        pltpu.make_async_copy(src, dst, in_sem.at[n])
        for n, (src, dst) in enumerate(
            ((k_in, k_v), (v_in, v_v), (q_in, q_v), (og_in, og_v), (w_in, w_v), (reach_in, reach))
        )
    ]
    for n in (5, 0, 1, 3, 4, 2):
        loads[n].start()

    barrier = pltpu.get_barrier_semaphore()

    def greet(device):
        pl.semaphore_signal(barrier, inc=1, device_id=device, device_id_type=MESH)

    for dy in (1, 2, 3):
        greet(at(ha_=lax.rem(ha + dy, 4)))
    greet(at(wa_=mate))
    greet(at(dp_=z_hi * 4 + x_one))
    greet(at(dp_=z_hi * 4 + x_three))

    def z_device(dz):
        zt = lax.rem(zi + dz, 8)
        return at(dp_=lax.div(zt, 4) * 4 + x, wa_=lax.rem(zt, 4) * 2 + core)

    for dz in range(1, 8):
        greet(z_device(dz))
    far_right = (core == 1) & has_right
    far_left = (core == 0) & has_left

    @pl.when(far_right)
    def _():
        greet(at(wa_=wa + 1))

    @pl.when(far_left)
    def _():
        greet(at(wa_=wa - 1))

    def columns(ref, head):
        return ref[:, head * HD : (head + 1) * HD]

    def slot_columns(ref, slot):
        return jnp.where(slot >= zero_head, columns(ref, slot + 1), columns(ref, slot))

    def zero_columns(ref):
        value = columns(ref, 0)
        for h in range(1, HEADS):
            value = jnp.where(zero_head == h, columns(ref, h), value)
        return value

    def head_value(of_slot, h):
        value = jnp.where(zero_head == h, of_slot(HALO), of_slot(min(h, HALO - 1)))
        return jnp.where(zero_head < h, of_slot(h - 1), value) if h else value

    @pl.when(wa == 0)
    def _():
        for buf in (kv, qa):
            def clear(s, carry, buf=buf):
                for kind in range(2):
                    for r in range(3):
                        buf[s, kind, r, 0] = jnp.zeros((TILE, HD), BF)
                return carry
            lax.fori_loop(0, HALO, clear, 0)
        for r in range(3):
            sb[r, 0] = jnp.zeros((TILE, HD), BF)

    @pl.when(wa == 7)
    def _():
        for buf in (kv, qa):
            def clear(s, carry, buf=buf):
                for kind in range(2):
                    for r in range(3):
                        buf[s, kind, r, 2] = jnp.zeros((TILE, HD), BF)
                return carry
            lax.fori_loop(0, HALO, clear, 0)
        for r in range(3):
            sb[r, 2] = jnp.zeros((TILE, HD), BF)

    loads[5].wait()

    zero_head = jnp.int32(0)
    for n in reversed(range(HEADS)):
        total = reach[n, 0]
        for t in range(1, 6):
            total = total + reach[n, t]
        zero_head = jnp.where(total == 0, n, zero_head)

    loads[0].wait()
    loads[1].wait()

    def place_own_kv():
        for s in range(HALO):
            kv[s, 0, 1, 1] = slot_columns(k_v, s)
            kv[s, 1, 1, 1] = slot_columns(v_v, s)
        kv0[0] = zero_columns(k_v)
        kv0[1] = zero_columns(v_v)

    place_own_kv()

    ha_up = lax.rem(ha + 3, 4)
    ha_down = lax.rem(ha + 1, 4)
    wa_right = jnp.minimum(wa + 1, 7)
    wa_left = jnp.maximum(wa - 1, 0)

    def y_copy(buf, send, recv, s, r):
        return pltpu.make_async_remote_copy(
            src_ref=buf.at[s, :, 1, 1], dst_ref=buf.at[s, :, r, 1],
            send_sem=send.at[s, r // 2], recv_sem=recv.at[s, r // 2],
            device_id=at(ha_=ha_up if r == 2 else ha_down), device_id_type=MESH,
        )

    def w_copy(buf, send, recv, s, r, c):
        return pltpu.make_async_remote_copy(
            src_ref=buf.at[s, :, r, 1], dst_ref=buf.at[s, :, r, c],
            send_sem=send.at[s, r, c // 2], recv_sem=recv.at[s, r, c // 2],
            device_id=at(wa_=wa_right if c == 0 else wa_left), device_id_type=MESH,
        )

    sends_to = {0: has_right, 2: has_left}
    gets_from = {0: has_left, 2: has_right}

    def w_send(buf, send, recv, s, r):
        for c in ANY_COLS:
            @pl.when(sends_to[c])
            def _(c=c):
                w_copy(buf, send, recv, s, r, c).start()

    def relay(buf, y_send, y_recv, w_s, w_r, s):
        for r in (0, 2):
            y_copy(buf, y_send, y_recv, s, r).wait_recv()
            w_send(buf, w_s, w_r, s, r)

    def w_wait(buf, send, recv, s):
        for c in ANY_COLS:
            @pl.when(gets_from[c])
            def _(c=c):
                for r in range(3):
                    w_copy(buf, send, recv, s, r, c).wait_recv()

    def relay_kv(s):
        relay(kv, yk_s, yk_r, wk_s, wk_r, s)

    def relay_qa(s):
        relay(qa, yq_s, yq_r, wq_s, wq_r, s)

    def wait_barrier():
        pl.semaphore_wait(barrier, 13 + (far_right | far_left).astype(jnp.int32))

    wait_barrier()

    def first_kv(s, carry):
        for r in (0, 2):
            y_copy(kv, yk_s, yk_r, s, r).start()
        w_send(kv, wk_s, wk_r, s, 1)
        return carry

    lax.fori_loop(0, HALO, first_kv, 0)

    def wait_loads():
        loads[2].wait()
        loads[3].wait()
        loads[4].wait()

    def amat():
        a_v[...] = dot(og_v[...], w_v[...]).astype(BF)

    def place_own_qa():
        for s in range(HALO):
            qa[s, 0, 1, 1] = slot_columns(q_v, s)
            qa[s, 1, 1, 1] = slot_columns(a_v, s)
            for r in (0, 2):
                y_copy(qa, yq_s, yq_r, s, r).start()
        qa0[0] = zero_columns(q_v)
        qa0[1] = zero_columns(a_v)

    eye = (
        lax.broadcasted_iota(jnp.int32, (HD, HD), 0) == lax.broadcasted_iota(jnp.int32, (HD, HD), 1)
    ).astype(F32).astype(BF)

    def transpose_og():
        for t in range(D // HD):
            ogt[t * HD : (t + 1) * HD, :] = dot_nt(eye, og_v[:, t * HD : (t + 1) * HD]).astype(BF)

    wait_loads()
    amat()
    place_own_qa()
    transpose_og()

    stat[...] = jnp.zeros((TILE, HD), F32)
    lane = lax.broadcasted_iota(jnp.int32, (ROWS, HD), 1)
    key_id = lax.broadcasted_iota(jnp.int32, (1, KEYS), 1)
    place = jnp.zeros((1, KEYS), jnp.int32)
    for n in range(1, 9):
        place = place + (key_id >= n * TILE).astype(jnp.int32)
    row_id = (key_id >= 3 * TILE).astype(jnp.int32) + (key_id >= 6 * TILE).astype(jnp.int32)
    col_id = place - 3 * row_id

    def bias_row(s, mirrored):
        later = s >= zero_head
        up, down, left, right = (jnp.where(later, reach[s + 1, t], reach[s, t]) for t in range(2, 6))
        if mirrored:
            up, down, left, right = down, up, right, left

        def bias(ok):
            return jnp.where(ok, 0.0, -jnp.inf).astype(F32)

        b_up = bias((up > 0) & (ha > 0))
        b_down = bias((down > 0) & (ha < 3))
        b_left = bias((left > 0) & has_left)
        b_right = bias((right > 0) & has_right)
        zero = jnp.zeros((1, KEYS), F32)
        by_row = jnp.where(row_id == 0, zero + b_up, jnp.where(row_id == 2, zero + b_down, zero))
        by_col = jnp.where(col_id == 0, zero + b_left, jnp.where(col_id == 2, zero + b_right, zero))
        return by_row + by_col

    def split3(value):
        high = value.astype(BF).astype(F32)
        rest = value - high
        mid = rest.astype(BF).astype(F32)
        return high, mid, rest - mid

    def forward(slot, q, a, k, v, bias):
        n = k.shape[0]
        s_buf[:, :n] = dot_nt(q, k)
        dp_buf[:, :n] = dot_nt(a, v)

        def rows_step(i, carry):
            rows = pl.ds(pl.multiple_of(i * ROWS, ROWS), ROWS)
            s = s_buf[rows, :n] * SCALE
            if bias is not None:
                s = s + bias
            d = dp_buf[rows, :n]
            peak = jnp.max(s, axis=1, keepdims=True)
            e = jnp.exp(s - peak)
            total = jnp.sum(e, axis=1, keepdims=True)
            p = e * (1.0 / total)
            delta = jnp.sum(p * d, axis=1, keepdims=True)
            p_buf[rows, :n] = p.astype(BF)
            ds_buf[rows, :n] = (p * (d - delta)).astype(BF)
            block = stat[rows, :]
            for base, parts in ((0, split3(peak + jnp.log(total))), (64, split3(delta))):
                for t, part in enumerate(parts):
                    block = jnp.where(lane == base + 3 * slot + t, part, block)
            stat[rows, :] = block
            return carry

        lax.fori_loop(0, TILE // ROWS, rows_step, 0, unroll=FORWARD_UNROLL if n == KEYS else True)
        att_buf[lax.rem(slot + 1, 2)] = dot(p_buf[:, :n], v).astype(BF)
        res[0, slot] = (dot(ds_buf[:, :n], k) * SCALE).astype(BF)

    def backward(slot, k, v, q, a, lse_row, delta_row):
        n = q.shape[0]
        s_buf[:, :n] = dot_nt(k, q)
        dp_buf[:, :n] = dot_nt(v, a)

        def rows_step(i, carry):
            rows = pl.ds(pl.multiple_of(i * ROWS, ROWS), ROWS)
            p = jnp.exp(s_buf[rows, :n] * SCALE - lse_row)
            p_buf[rows, :n] = p.astype(BF)
            ds_buf[rows, :n] = (p * (dp_buf[rows, :n] - delta_row)).astype(BF)
            return carry

        lax.fori_loop(0, TILE // ROWS, rows_step, 0)
        res[2, slot] = dot(p_buf[:, :n], a).astype(BF)
        res[1, slot] = (dot(ds_buf[:, :n], q) * SCALE).astype(BF)

    def weight_term(pair):
        attended = jnp.concatenate([att_buf[0], att_buf[1]], axis=1)
        for t in range(8):
            both = dot(ogt[t * 192 : (t + 1) * 192, :], attended).astype(BF)
            gbuf[2 * pair, t // 4, t % 4] = both[:, :HD]
            gbuf[2 * pair + 1, t // 4, t % 4] = both[:, HD:]

    def mate_copy(j):
        return pltpu.make_async_remote_copy(
            src_ref=gbuf.at[2 * j + 1 - core], dst_ref=rbuf.at[j],
            send_sem=dd_s.at[j], recv_sem=dd_r.at[j], device_id=at(wa_=mate), device_id_type=MESH,
        )

    def x1_copy(j, which):
        return pltpu.make_async_remote_copy(
            src_ref=abuf.at[j, :, x_far if which else x_a], dst_ref=x1buf.at[j, which],
            send_sem=x1_s.at[j, which], recv_sem=x1_r.at[j, which],
            device_id=at(dp_=z_hi * 4 + x_a), device_id_type=MESH,
        )

    def x2_copy(j):
        return pltpu.make_async_remote_copy(
            src_ref=xs.at[j], dst_ref=x2buf.at[j],
            send_sem=x2_s.at[j], recv_sem=x2_r.at[j],
            device_id=at(dp_=z_hi * 4 + x_b), device_id_type=MESH,
        )

    def y_sum_copy(j, dy):
        to = lax.rem(ha + dy, 4)
        return pltpu.make_async_remote_copy(
            src_ref=cbuf.at[j, :, to], dst_ref=ybuf.at[dy - 1, j],
            send_sem=yy_s.at[j, dy - 1], recv_sem=yy_r.at[j, dy - 1],
            device_id=at(ha_=to), device_id_type=MESH,
        )

    def z_sum_copy(dz):
        return pltpu.make_async_remote_copy(
            src_ref=zbuf.at[:, lax.rem(zi + dz, 8)], dst_ref=zr.at[dz - 1],
            send_sem=zz_s.at[dz - 1], recv_sem=zz_r.at[dz - 1],
            device_id=z_device(dz), device_id_type=MESH,
        )

    def last_copy():
        return pltpu.make_async_remote_copy(
            src_ref=fbuf.at[:, 1 - core], dst_ref=f2, send_sem=fin_s.at[0], recv_sem=fin_r.at[0],
            device_id=at(wa_=mate), device_id_type=MESH,
        )

    def wide(value):
        return value.astype(F32)

    def add_mate(j):
        mate_copy(j).wait_recv()

        def add(at_x):
            for h in range(2):
                abuf[j, h, at_x] = (
                    wide(gbuf[2 * j + core, h, at_x]) + wide(rbuf[j, h, at_x])
                ).astype(BF)

        add(x_far)
        x1_copy(j, 1).start()
        add(x_a)
        x1_copy(j, 0).start()
        add(x_b)
        add(x)

    def add_x1(j):
        x1_copy(j, 1).wait_recv()
        for h in range(2):
            xs[j, h] = (wide(abuf[j, h, x_b]) + wide(x1buf[j, 1, h])).astype(BF)
        x2_copy(j).start()

    def add_x2(j):
        x1_copy(j, 0).wait_recv()
        x2_copy(j).wait_recv()
        for h in range(2):
            total = wide(abuf[j, h, x]) + wide(x1buf[j, 0, h]) + wide(x2buf[j, h])
            cbuf[j, h] = total.astype(BF).reshape(4, 48, HD)
        for dy in (2, 1, 3):
            y_sum_copy(j, dy).start()

    pick = (lax.broadcasted_iota(jnp.int32, (128, 96), 0), lax.broadcasted_iota(jnp.int32, (128, 96), 1))

    spread = (
        ((pick[0] & 7) < 6) & (pick[1] == (pick[0] >> 3) * 6 + (pick[0] & 7))
    ).astype(F32).astype(BF)

    def add_y(j):
        for dy in (1, 2, 3):
            y_sum_copy(j, dy).wait_recv()
        halves = []
        for h in range(2):
            total = wide(cbuf[j, h, ha])
            for n in range(3):
                total = total + wide(ybuf[n, j, h])
            halves.append(total.astype(BF))
        rows = dot(spread, jnp.concatenate(halves, axis=0))
        zbuf[j] = rows.astype(BF).reshape(8, 16, HD)

    def send_z():
        for dz in (4, 3, 5, 2, 6, 1, 7):
            z_sum_copy(dz).start()

    def add_z():
        for dz in range(1, 8):
            z_sum_copy(dz).wait_recv()
        for j in range(3):
            total = wide(zbuf[j, zi])
            for n in range(7):
                total = total + wide(zr[n, j])
            fbuf[j] = total.reshape(2, 8, HD)
        last_copy().start()

    def finish_weights():
        last_copy().wait_recv()
        for j in range(3):
            gws[2 * j + core] = fbuf[j, core]
            gws[2 * j + 1 - core] = f2[j]
        for h in range(HEADS):
            gw_out[:, h * HD : (h + 1) * HD] = head_value(lambda s: gws[(s + 1) % HEADS, 0:6, :], h)

    def own_qa():
        def step(t, c):
            w_send(qa, wq_s, wq_r, t, 1)
            return c

        lax.fori_loop(0, HALO, step, 0)

    def hooked(s, hooks):
        for n, ops in hooks.items():
            @pl.when(s == n)
            def _(ops=ops):
                for op, *args in ops:
                    op(*args)

    def pair_done(pair):
        weight_term(pair)
        mate_copy(pair).start()

    forward(HALO, qa0[0], qa0[1], kv0[0], kv0[1], None)
    relay_kv(0)
    relay_kv(1)

    def forward_step(s, carry):
        hooked(s, BEFORE_FORWARD)
        w_wait(kv, wk_s, wk_r, s)
        forward(
            s, qa[s, 0, 1, 1], qa[s, 1, 1, 1],
            kv[s, 0].reshape(KEYS, HD), kv[s, 1].reshape(KEYS, HD), bias_row(s, False),
        )
        hooked(s, AFTER_FORWARD)
        return carry

    BEFORE_FORWARD = {
        0: [(relay_kv, 2)],
        1: [(relay_kv, 3)],
        2: [(relay_kv, 4), (own_qa,)],
        3: [(relay_qa, 0)],
        4: [(relay_qa, 1)],
    }
    AFTER_FORWARD = {
        0: [(pair_done, 0)],
        2: [(pair_done, 1)],
        3: [(add_mate, 0)],
        4: [(pair_done, 2)],
    }
    lax.fori_loop(0, HALO, forward_step, 0)

    sb[1, 1] = stat[...].astype(BF)

    def sy_copy(r):
        return pltpu.make_async_remote_copy(
            src_ref=sb.at[1, 1], dst_ref=sb.at[r, 1], send_sem=sy_s.at[r // 2], recv_sem=sy_r.at[r // 2],
            device_id=at(ha_=ha_up if r == 2 else ha_down), device_id_type=MESH,
        )

    def sw_copy(r, c):
        return pltpu.make_async_remote_copy(
            src_ref=sb.at[r, 1], dst_ref=sb.at[r, c],
            send_sem=sw_s.at[r, c // 2], recv_sem=sw_r.at[r, c // 2],
            device_id=at(wa_=wa_right if c == 0 else wa_left), device_id_type=MESH,
        )

    def sw_send(r):
        for c in ANY_COLS:
            @pl.when(sends_to[c])
            def _(c=c):
                sw_copy(r, c).start()

    for r in (0, 2):
        sy_copy(r).start()
    sw_send(1)
    relay_qa(2)
    add_mate(1)
    add_x1(0)

    chosen = (lax.broadcasted_iota(jnp.int32, (16, HD), 0), lax.broadcasted_iota(jnp.int32, (16, HD), 1))
    first = (chosen[0] & 7) * 3 + (chosen[0] >> 3) * 64
    take = ((chosen[1] >= first) & (chosen[1] < first + 3) & ((chosen[0] & 7) < 6)).astype(F32).astype(BF)

    relay_qa(3)
    own = dot_nt(take, sb[1, 1])
    backward(
        HALO, kv0[0], kv0[1], qa0[0], qa0[1], own[HALO : HALO + 1, :], own[8 + HALO : 9 + HALO, :]
    )
    add_mate(2)

    def relay_stats():
        for r in (0, 2):
            sy_copy(r).wait_recv()
            sw_send(r)

    relay_stats()
    relay_qa(4)
    add_x1(1)
    add_x2(0)

    def wait_stats():
        for c in ANY_COLS:
            @pl.when(gets_from[c])
            def _(c=c):
                for r in range(3):
                    sw_copy(r, c).wait_recv()

    add_x1(2)
    wait_stats()
    trow[...] = dot_nt(take, sb[...].reshape(KEYS, HD))

    def backward_step(s, carry):
        w_wait(qa, wq_s, wq_r, s)
        backward(
            s, kv[s, 0, 1, 1], kv[s, 1, 1, 1], qa[s, 0].reshape(KEYS, HD), qa[s, 1].reshape(KEYS, HD),
            trow[pl.ds(s, 1), :] - bias_row(s, True), trow[pl.ds(s + 8, 1), :],
        )
        hooked(s, AFTER_BACKWARD)
        return carry

    AFTER_BACKWARD = {
        0: [(add_x2, 1), (add_x2, 2)],
        1: [(add_y, 0)],
        2: [(add_y, 1), (add_y, 2), (send_z,)],
    }
    lax.fori_loop(0, HALO, backward_step, 0)

    def place_outputs():
        for h in range(HEADS):
            cols = slice(h * HD, (h + 1) * HD)
            for n in range(3):
                grads_out[n, :, cols] = head_value(lambda s: res[n, s], h)

    place_outputs()
    add_z()
    finish_weights()

    def sent(s, carry):
        for r in (0, 2):
            y_copy(kv, yk_s, yk_r, s, r).wait_send()
            y_copy(qa, yq_s, yq_r, s, r).wait_send()
        for c in ANY_COLS:
            @pl.when(sends_to[c])
            def _(c=c):
                for r in range(3):
                    w_copy(kv, wk_s, wk_r, s, r, c).wait_send()
                    w_copy(qa, wq_s, wq_r, s, r, c).wait_send()
        return carry

    lax.fori_loop(0, HALO, sent, 0)
    for r in (0, 2):
        sy_copy(r).wait_send()
    for c in ANY_COLS:
        @pl.when(sends_to[c])
        def _(c=c):
            for r in range(3):
                sw_copy(r, c).wait_send()
    for j in range(3):
        mate_copy(j).wait_send()
        x1_copy(j, 0).wait_send()
        x1_copy(j, 1).wait_send()
        x2_copy(j).wait_send()
    for j in range(3):
        for dy in (1, 2, 3):
            y_sum_copy(j, dy).wait_send()
    for dz in range(1, 8):
        z_sum_copy(dz).wait_send()
    last_copy().wait_send()


def put_out(grads, gw, gq_out, gk_out, gv_out, gw_out, sem):
    copies = [
        pltpu.make_async_copy(grads.at[n], ref, sem.at[n]) for n, ref in enumerate((gq_out, gk_out, gv_out))
    ]
    copies.append(pltpu.make_async_copy(gw, gw_out, sem.at[3]))
    for copy in copies:
        copy.start()
    for copy in copies:
        copy.wait()


def shards(queries, key_tiles, value_tiles, out_grad, w_out, reaches):
    dma = pltpu.SemaphoreType.DMA
    vm = pltpu.VMEM
    shapes = [
        pltpu.SMEM((HEADS, 6), jnp.int32),
        vm((TILE, HQ), BF), vm((TILE, HQ), BF), vm((TILE, HQ), BF), vm((TILE, D), BF), vm((D, HQ), BF),
        vm((TILE, HQ), BF), vm((D, TILE), BF),
        vm((HALO, 2, 3, 3, TILE, HD), BF), vm((HALO, 2, 3, 3, TILE, HD), BF),
        vm((2, TILE, HD), BF), vm((2, TILE, HD), BF),
        vm((TILE, HD), F32), vm((3, 3, TILE, HD), BF), vm((16, KEYS), F32),
        vm((TILE, KEYS), F32), vm((TILE, KEYS), F32), vm((TILE, KEYS), BF), vm((TILE, KEYS), BF),
        vm((2, TILE, HD), BF), vm((3, HEADS, TILE, HD), BF),
        vm((6, 2, 4, 192, HD), BF), vm((3, 2, 4, 192, HD), BF), vm((3, 2, 4, 192, HD), BF),
        vm((3, 2, 2, 192, HD), BF), vm((3, 2, 192, HD), BF), vm((3, 2, 192, HD), BF),
        vm((3, 2, 4, 48, HD), BF), vm((3, 3, 2, 48, HD), BF),
        vm((3, 8, 16, HD), BF), vm((7, 3, 16, HD), BF),
        vm((3, 2, 8, HD), F32), vm((3, 8, HD), F32), vm((6, 8, HD), F32),
        dma((6,)),
    ]
    for extent in ((HALO, 2), (HALO, 2), (HALO, 3, 2), (HALO, 3, 2), (2,), (3, 2), (3,), (3, 2), (3,), (3, 3), (7,), (1,)):
        shapes += [dma(extent), dma(extent)]
    anywhere = pl.BlockSpec(memory_space=pl.ANY)
    inside = pl.BlockSpec(memory_space=pltpu.VMEM)
    grads, gw = pl.pallas_call(
        kernel,
        out_shape=(pltpu.VMEM((3, TILE, HQ), BF), pltpu.VMEM((6, HQ), F32)),
        in_specs=[anywhere] * 6,
        out_specs=(inside,) * 2,
        scratch_shapes=shapes,
        compiler_params=pltpu.CompilerParams(collective_id=0, has_side_effects=True),
    )(
        reaches,
        queries.reshape(TILE, HQ),
        key_tiles.reshape(TILE, HQ),
        value_tiles.reshape(TILE, HQ),
        out_grad.reshape(TILE, D),
        w_out,
    )
    tile = jax.ShapeDtypeStruct((TILE, HQ), BF)
    gq, gk, gv, gw = pl.pallas_call(
        put_out,
        out_shape=(tile, tile, tile, jax.ShapeDtypeStruct((6, HQ), F32)),
        in_specs=[inside] * 2,
        out_specs=(anywhere,) * 4,
        scratch_shapes=[dma((4,))],
    )(*(pltpu.with_memory_space_constraint(value, pltpu.VMEM) for value in (grads, gw)))
    return gq.reshape(queries.shape), gk.reshape(queries.shape), gv.reshape(queries.shape), gw


def solution(mesh):
    tiles = P("dp", None, "ha", "wa", None, None)
    return jax.shard_map(
        shards,
        mesh=mesh,
        in_specs=(tiles, tiles, tiles, tiles, P(), P()),
        out_specs=(tiles, tiles, tiles, P(("dp", "ha", "wa"), None)),
        check_vma=False,
    )
```

```python
import math

import jax
import jax.numpy as jnp
from jax import lax
from jax.experimental import pallas as pl
from jax.experimental.pallas import tpu as pltpu
from jax.sharding import PartitionSpec as P

MESH = pl.DeviceIdType.MESH
HEADS = 6
HALO = 5
HD = 128
TILE = 144
KEYS = 9 * TILE
HQ = HEADS * HD
D = 1536
SCALE = 1.0 / math.sqrt(HD)
ROWS = 16
FORWARD_UNROLL = 9
BF = jnp.bfloat16
F32 = jnp.float32
ANY_COLS = (0, 2)


def dot(a, b):
    return jnp.dot(a, b, preferred_element_type=F32)


def dot_nt(a, b):
    return lax.dot_general(a, b, (((1,), (1,)), ((), ())), preferred_element_type=F32)


def kernel(
    reach_in, q_in, k_in, v_in, og_in, w_in,
    grads_out, gw_out,
    reach, q_v, k_v, v_v, og_v, w_v, a_v, ogt, kv, qa, kv0, qa0, stat, sb, trow,
    s_buf, dp_buf, p_buf, ds_buf, att_buf, res,
    gbuf, rbuf, abuf, x1buf, xs, x2buf, cbuf, ybuf, zbuf, zr, gws,
    in_sem, yk_s, yk_r, yq_s, yq_r, wk_s, wk_r, wq_s, wq_r, sy_s, sy_r, sw_s, sw_r,
    dd_s, dd_r, x1_s, x1_r, x2_s, x2_r, yy_s, yy_r, zz_s, zz_r,
):
    dp = lax.axis_index("dp")
    ha = lax.axis_index("ha")
    wa = lax.axis_index("wa")
    x = lax.rem(dp, 4)
    z_hi = lax.div(dp, 4)
    core = lax.rem(wa, 2)
    z_lo = lax.div(wa, 2)
    zi = z_hi * 4 + z_lo
    mate = wa + 1 - 2 * core
    x_one = x + 1 - 2 * lax.rem(x, 2)
    x_three = 3 - x
    x_far = lax.rem(x + 2, 4)
    x_a = x_one + core * (x_three - x_one)
    x_b = x_three + core * (x_one - x_three)
    has_left = wa > 0
    has_right = wa < 7

    def at(dp_=dp, ha_=ha, wa_=wa):
        return (dp_, ha_, wa_)

    loads = [
        pltpu.make_async_copy(src, dst, in_sem.at[n])
        for n, (src, dst) in enumerate(
            ((k_in, k_v), (v_in, v_v), (q_in, q_v), (og_in, og_v), (w_in, w_v), (reach_in, reach))
        )
    ]
    for n in (5, 0, 1, 3, 4, 2):
        loads[n].start()

    barrier = pltpu.get_barrier_semaphore()

    def greet(device):
        pl.semaphore_signal(barrier, inc=1, device_id=device, device_id_type=MESH)

    for dy in (1, 2, 3):
        greet(at(ha_=lax.rem(ha + dy, 4)))
    greet(at(wa_=mate))
    greet(at(dp_=z_hi * 4 + x_one))
    greet(at(dp_=z_hi * 4 + x_three))

    def z_target(shift, other):
        zl = lax.rem(z_lo + shift, 4)
        to_core = 1 - core if other else core
        return at(dp_=core * 4 + x, wa_=zl * 2 + to_core)

    for dz in range(1, 8):
        zt = lax.rem(zi + dz, 8)
        greet(at(dp_=lax.div(zt, 4) * 4 + x, wa_=lax.rem(zt, 4) * 2 + z_hi))
    own_z = z_hi == core
    far_right = (core == 1) & has_right
    far_left = (core == 0) & has_left

    @pl.when(far_right)
    def _():
        greet(at(wa_=wa + 1))

    @pl.when(far_left)
    def _():
        greet(at(wa_=wa - 1))

    def columns(ref, head):
        return ref[:, head * HD : (head + 1) * HD]

    def slot_columns(ref, slot):
        return jnp.where(slot >= zero_head, columns(ref, slot + 1), columns(ref, slot))

    def zero_columns(ref):
        value = columns(ref, 0)
        for h in range(1, HEADS):
            value = jnp.where(zero_head == h, columns(ref, h), value)
        return value

    def head_value(of_slot, h):
        value = jnp.where(zero_head == h, of_slot(HALO), of_slot(min(h, HALO - 1)))
        return jnp.where(zero_head < h, of_slot(h - 1), value) if h else value

    @pl.when(wa == 0)
    def _():
        for buf in (kv, qa):
            def clear(s, carry, buf=buf):
                for kind in range(2):
                    for r in range(3):
                        buf[s, kind, r, 0] = jnp.zeros((TILE, HD), BF)
                return carry
            lax.fori_loop(0, HALO, clear, 0)
        for r in range(3):
            sb[r, 0] = jnp.zeros((TILE, HD), BF)

    @pl.when(wa == 7)
    def _():
        for buf in (kv, qa):
            def clear(s, carry, buf=buf):
                for kind in range(2):
                    for r in range(3):
                        buf[s, kind, r, 2] = jnp.zeros((TILE, HD), BF)
                return carry
            lax.fori_loop(0, HALO, clear, 0)
        for r in range(3):
            sb[r, 2] = jnp.zeros((TILE, HD), BF)

    loads[5].wait()

    zero_head = jnp.int32(0)
    for n in reversed(range(HEADS)):
        total = reach[n, 0]
        for t in range(1, 6):
            total = total + reach[n, t]
        zero_head = jnp.where(total == 0, n, zero_head)

    loads[0].wait()
    loads[1].wait()

    def place_own_kv():
        for s in range(HALO):
            kv[s, 0, 1, 1] = slot_columns(k_v, s)
            kv[s, 1, 1, 1] = slot_columns(v_v, s)
        kv0[0] = zero_columns(k_v)
        kv0[1] = zero_columns(v_v)

    place_own_kv()

    ha_up = lax.rem(ha + 3, 4)
    ha_down = lax.rem(ha + 1, 4)
    wa_right = jnp.minimum(wa + 1, 7)
    wa_left = jnp.maximum(wa - 1, 0)

    def y_copy(buf, send, recv, s, r):
        return pltpu.make_async_remote_copy(
            src_ref=buf.at[s, :, 1, 1], dst_ref=buf.at[s, :, r, 1],
            send_sem=send.at[r // 2], recv_sem=recv.at[s, r // 2],
            device_id=at(ha_=ha_up if r == 2 else ha_down), device_id_type=MESH,
        )

    def w_copy(buf, send, recv, s, r, c):
        return pltpu.make_async_remote_copy(
            src_ref=buf.at[s, :, r, 1], dst_ref=buf.at[s, :, r, c],
            send_sem=send.at[c // 2], recv_sem=recv.at[s, c // 2],
            device_id=at(wa_=wa_right if c == 0 else wa_left), device_id_type=MESH,
        )

    sends_to = {0: has_right, 2: has_left}
    gets_from = {0: has_left, 2: has_right}

    def w_send(buf, send, recv, s, r):
        for c in ANY_COLS:
            @pl.when(sends_to[c])
            def _(c=c):
                w_copy(buf, send, recv, s, r, c).start()

    def relay(buf, y_send, y_recv, w_s, w_r, s):
        for r in (0, 2):
            y_copy(buf, y_send, y_recv, s, r).wait_recv()
            w_send(buf, w_s, w_r, s, r)

    def w_wait(buf, send, recv, s):
        for c in ANY_COLS:
            @pl.when(gets_from[c])
            def _(c=c):
                pltpu.make_async_copy(buf.at[s, :, :, 1], buf.at[s, :, :, c], recv.at[s, c // 2]).wait()

    def relay_kv(s):
        relay(kv, yk_s, yk_r, wk_s, wk_r, s)

    def relay_qa(s):
        relay(qa, yq_s, yq_r, wq_s, wq_r, s)

    def wait_barrier():
        pl.semaphore_wait(barrier, 14 - 2 * own_z.astype(jnp.int32) + (far_right | far_left).astype(jnp.int32))

    wait_barrier()

    def first_kv(s, carry):
        for r in (0, 2):
            y_copy(kv, yk_s, yk_r, s, r).start()
        w_send(kv, wk_s, wk_r, s, 1)
        return carry

    lax.fori_loop(0, HALO, first_kv, 0)

    def wait_loads():
        loads[2].wait()
        loads[3].wait()
        loads[4].wait()

    def amat():
        a_v[...] = dot(og_v[...], w_v[...]).astype(BF)

    def place_own_qa():
        for s in range(HALO):
            qa[s, 0, 1, 1] = slot_columns(q_v, s)
            qa[s, 1, 1, 1] = slot_columns(a_v, s)
            for r in (0, 2):
                y_copy(qa, yq_s, yq_r, s, r).start()
        qa0[0] = zero_columns(q_v)
        qa0[1] = zero_columns(a_v)

    eye = (
        lax.broadcasted_iota(jnp.int32, (HD, HD), 0) == lax.broadcasted_iota(jnp.int32, (HD, HD), 1)
    ).astype(F32).astype(BF)

    def transpose_og():
        for t in range(D // HD):
            ogt[t * HD : (t + 1) * HD, :] = dot_nt(eye, og_v[:, t * HD : (t + 1) * HD]).astype(BF)

    wait_loads()
    amat()
    place_own_qa()
    transpose_og()

    stat[...] = jnp.zeros((TILE, HD), F32)
    lane = lax.broadcasted_iota(jnp.int32, (ROWS, HD), 1)
    key_id = lax.broadcasted_iota(jnp.int32, (1, KEYS), 1)
    place = jnp.zeros((1, KEYS), jnp.int32)
    for n in range(1, 9):
        place = place + (key_id >= n * TILE).astype(jnp.int32)
    row_id = (key_id >= 3 * TILE).astype(jnp.int32) + (key_id >= 6 * TILE).astype(jnp.int32)
    col_id = place - 3 * row_id

    def bias_row(s, mirrored):
        later = s >= zero_head
        up, down, left, right = (jnp.where(later, reach[s + 1, t], reach[s, t]) for t in range(2, 6))
        if mirrored:
            up, down, left, right = down, up, right, left

        def bias(ok):
            return jnp.where(ok, 0.0, -jnp.inf).astype(F32)

        b_up = bias((up > 0) & (ha > 0))
        b_down = bias((down > 0) & (ha < 3))
        b_left = bias((left > 0) & has_left)
        b_right = bias((right > 0) & has_right)
        zero = jnp.zeros((1, KEYS), F32)
        by_row = jnp.where(row_id == 0, zero + b_up, jnp.where(row_id == 2, zero + b_down, zero))
        by_col = jnp.where(col_id == 0, zero + b_left, jnp.where(col_id == 2, zero + b_right, zero))
        return by_row + by_col

    def split3(value):
        high = value.astype(BF).astype(F32)
        rest = value - high
        mid = rest.astype(BF).astype(F32)
        return high, mid, rest - mid

    def forward(slot, q, a, k, v, bias):
        n = k.shape[0]
        s_buf[:, :n] = dot_nt(q, k)
        dp_buf[:, :n] = dot_nt(a, v)

        def rows_step(i, carry):
            rows = pl.ds(pl.multiple_of(i * ROWS, ROWS), ROWS)
            s = s_buf[rows, :n] * SCALE
            if bias is not None:
                s = s + bias
            d = dp_buf[rows, :n]
            peak = jnp.max(s, axis=1, keepdims=True)
            e = jnp.exp(s - peak)
            total = jnp.sum(e, axis=1, keepdims=True)
            p = e * (1.0 / total)
            delta = jnp.sum(p * d, axis=1, keepdims=True)
            p_buf[rows, :n] = p.astype(BF)
            ds_buf[rows, :n] = (p * (d - delta)).astype(BF)
            block = stat[rows, :]
            for base, parts in ((0, split3(peak + jnp.log(total))), (64, split3(delta))):
                for t, part in enumerate(parts):
                    block = jnp.where(lane == base + 3 * slot + t, part, block)
            stat[rows, :] = block
            return carry

        lax.fori_loop(0, TILE // ROWS, rows_step, 0, unroll=FORWARD_UNROLL if n == KEYS else True)
        att_buf[lax.rem(slot + 1, 2)] = dot(p_buf[:, :n], v).astype(BF)
        res[0, slot] = (dot(ds_buf[:, :n], k) * SCALE).astype(BF)

    def backward(slot, k, v, q, a, lse_row, delta_row):
        n = q.shape[0]
        s_buf[:, :n] = dot_nt(k, q)
        dp_buf[:, :n] = dot_nt(v, a)

        def rows_step(i, carry):
            rows = pl.ds(pl.multiple_of(i * ROWS, ROWS), ROWS)
            p = jnp.exp(s_buf[rows, :n] * SCALE - lse_row)
            p_buf[rows, :n] = p.astype(BF)
            ds_buf[rows, :n] = (p * (dp_buf[rows, :n] - delta_row)).astype(BF)
            return carry

        lax.fori_loop(0, TILE // ROWS, rows_step, 0)
        res[2, slot] = dot(p_buf[:, :n], a).astype(BF)
        res[1, slot] = (dot(ds_buf[:, :n], q) * SCALE).astype(BF)

    GROUPS = ((0, 2), (2, 2), (4, 1), (5, 1))

    def units(group):
        return pl.ds(*GROUPS[group])

    def weight_term(group):
        unit, count = GROUPS[group]
        if count == 2:
            attended = jnp.concatenate([att_buf[0], att_buf[1]], axis=1)
        else:
            attended = att_buf[unit % 2]
        for t in range(8):
            both = dot(ogt[t * 192 : (t + 1) * 192, :], attended).astype(BF)
            for n in range(count):
                gbuf[unit + n, t // 4, t % 4] = both[:, n * HD : (n + 1) * HD]

    def mate_copy(g):
        return pltpu.make_async_remote_copy(
            src_ref=gbuf.at[units(g), 1 - core], dst_ref=rbuf.at[units(g)],
            send_sem=dd_s.at[0], recv_sem=dd_r.at[g], device_id=at(wa_=mate), device_id_type=MESH,
        )

    def x1_copy(g, which):
        return pltpu.make_async_remote_copy(
            src_ref=abuf.at[units(g), x_far if which else x_a], dst_ref=x1buf.at[which, units(g)],
            send_sem=x1_s.at[0], recv_sem=x1_r.at[g, which],
            device_id=at(dp_=z_hi * 4 + x_a), device_id_type=MESH,
        )

    def x2_copy(g):
        return pltpu.make_async_remote_copy(
            src_ref=xs.at[units(g)], dst_ref=x2buf.at[units(g)],
            send_sem=x2_s.at[0], recv_sem=x2_r.at[g],
            device_id=at(dp_=z_hi * 4 + x_b), device_id_type=MESH,
        )

    def y_sum_copy(g, dy):
        to = lax.rem(ha + dy, 4)
        return pltpu.make_async_remote_copy(
            src_ref=cbuf.at[units(g), to], dst_ref=ybuf.at[dy - 1, units(g)],
            send_sem=yy_s.at[0], recv_sem=yy_r.at[g],
            device_id=at(ha_=to), device_id_type=MESH,
        )

    Z_GROUPS = ((0, 2), (2, 1))

    def z_sum_copy(n, shift, other):
        target = lax.rem(z_lo + shift, 4) * 2 + (1 - core if other else core)
        return pltpu.make_async_remote_copy(
            src_ref=zbuf.at[target, pl.ds(*Z_GROUPS[n])],
            dst_ref=zr.at[z_hi * 4 + shift, pl.ds(*Z_GROUPS[n])],
            send_sem=zz_s.at[0], recv_sem=zz_r.at[n],
            device_id=z_target(shift, other), device_id_type=MESH,
        )

    def wide(value):
        return value.astype(F32)

    def unit_range(g):
        return range(GROUPS[g][0], GROUPS[g][0] + GROUPS[g][1])

    def add_mate(g):
        mate_copy(g).wait_recv()

        def add(at_x):
            for u in unit_range(g):
                abuf[u, at_x] = (wide(gbuf[u, core, at_x]) + wide(rbuf[u, at_x])).astype(BF)

        add(x_far)
        x1_copy(g, 1).start()
        add(x_a)
        x1_copy(g, 0).start()
        add(x_b)
        add(x)

    def add_x1(g):
        x1_copy(g, 1).wait_recv()
        for u in unit_range(g):
            xs[u] = (wide(abuf[u, x_b]) + wide(x1buf[1, u])).astype(BF)
        x2_copy(g).start()

    def add_x2(g):
        x1_copy(g, 0).wait_recv()
        x2_copy(g).wait_recv()
        for u in unit_range(g):
            total = wide(abuf[u, x]) + wide(x1buf[0, u]) + wide(x2buf[u])
            cbuf[u] = total.astype(BF).reshape(4, 48, HD)
        for dy in (2, 1, 3):
            y_sum_copy(g, dy).start()

    def wait_y(g):
        pltpu.make_async_copy(ybuf.at[:, units(g)], ybuf.at[:, units(g)], yy_r.at[g]).wait()

    pick = (lax.broadcasted_iota(jnp.int32, (128, 96), 0), lax.broadcasted_iota(jnp.int32, (128, 96), 1))
    spread = (
        ((pick[0] & 7) < 6)
        & (pick[1] == ((pick[0] >> 3) & 1) * 48 + (pick[0] >> 4) * 6 + (pick[0] & 7))
    ).astype(F32).astype(BF)

    def add_y(pair):
        halves = []
        for u in (2 * pair, 2 * pair + 1):
            total = wide(cbuf[u, ha])
            for n in range(3):
                total = total + wide(ybuf[n, u])
            halves.append(total.astype(BF))
        rows = dot(spread, jnp.concatenate(halves, axis=0))
        zbuf[:, pair] = rows.astype(BF).reshape(8, 16, HD)

    def send_z(n):
        for shift in (2, 1, 3, 0):
            z_sum_copy(n, shift, True).start()
            if shift:
                z_sum_copy(n, shift, False).start()

        @pl.when(jnp.logical_not(own_z))
        def _():
            z_sum_copy(n, 0, False).start()

        @pl.when(own_z)
        def _():
            pairs = range(Z_GROUPS[n][0], Z_GROUPS[n][0] + Z_GROUPS[n][1])
            for pair in pairs:
                zr[zi - z_lo, pair] = zbuf[z_lo * 2 + core, pair]

    def z_bytes(ref, count, n):
        part = ref.at[0:count, pl.ds(*Z_GROUPS[n])]
        return part, part

    def add_z():
        for n in range(2):
            @pl.when(own_z)
            def _(n=n):
                pltpu.make_async_copy(*z_bytes(zr, 7, n), zz_r.at[n]).wait()

            @pl.when(jnp.logical_not(own_z))
            def _(n=n):
                pltpu.make_async_copy(*z_bytes(zr, 8, n), zz_r.at[n]).wait()
        for pair in range(3):
            total = wide(zr[0, pair])
            for n in range(1, 8):
                total = total + wide(zr[n, pair])
            gws[2 * pair] = total[:8]
            gws[2 * pair + 1] = total[8:]
        for h in range(HEADS):
            gw_out[:, h * HD : (h + 1) * HD] = head_value(lambda s: gws[(s + 1) % HEADS, 0:6, :], h)

    def own_qa():
        def step(t, c):
            w_send(qa, wq_s, wq_r, t, 1)
            return c

        lax.fori_loop(0, HALO, step, 0)

    def hooked(s, hooks):
        for n, ops in hooks.items():
            @pl.when(s == n)
            def _(ops=ops):
                for op, *args in ops:
                    op(*args)

    def group_done(g):
        weight_term(g)
        mate_copy(g).start()

    forward(HALO, qa0[0], qa0[1], kv0[0], kv0[1], None)
    relay_kv(0)
    relay_kv(1)

    def forward_step(s, carry):
        hooked(s, BEFORE_FORWARD)
        w_wait(kv, wk_s, wk_r, s)
        forward(
            s, qa[s, 0, 1, 1], qa[s, 1, 1, 1],
            kv[s, 0].reshape(KEYS, HD), kv[s, 1].reshape(KEYS, HD), bias_row(s, False),
        )
        hooked(s, AFTER_FORWARD)
        return carry

    BEFORE_FORWARD = {
        0: [(relay_kv, 2)],
        1: [(relay_kv, 3)],
        2: [(relay_kv, 4), (own_qa,)],
        3: [(relay_qa, 0)],
        4: [(relay_qa, 1)],
    }
    AFTER_FORWARD = {
        0: [(group_done, 0)],
        2: [(group_done, 1), (add_mate, 0)],
        3: [(group_done, 2)],
        4: [(group_done, 3)],
    }
    lax.fori_loop(0, HALO, forward_step, 0)

    sb[1, 1] = stat[...].astype(BF)

    def sy_copy(r):
        return pltpu.make_async_remote_copy(
            src_ref=sb.at[1, 1], dst_ref=sb.at[r, 1], send_sem=sy_s.at[0], recv_sem=sy_r.at[r // 2],
            device_id=at(ha_=ha_up if r == 2 else ha_down), device_id_type=MESH,
        )

    def sw_copy(r, c):
        return pltpu.make_async_remote_copy(
            src_ref=sb.at[r, 1], dst_ref=sb.at[r, c],
            send_sem=sw_s.at[c // 2], recv_sem=sw_r.at[c // 2],
            device_id=at(wa_=wa_right if c == 0 else wa_left), device_id_type=MESH,
        )

    def sw_send(r):
        for c in ANY_COLS:
            @pl.when(sends_to[c])
            def _(c=c):
                sw_copy(r, c).start()

    chosen = (lax.broadcasted_iota(jnp.int32, (16, HD), 0), lax.broadcasted_iota(jnp.int32, (16, HD), 1))
    first = (chosen[0] & 7) * 3 + (chosen[0] >> 3) * 64
    take = ((chosen[1] >= first) & (chosen[1] < first + 3) & ((chosen[0] & 7) < 6)).astype(F32).astype(BF)

    def relay_stats():
        for r in (0, 2):
            sy_copy(r).wait_recv()
            sw_send(r)

    def wait_stats():
        for c in ANY_COLS:
            @pl.when(gets_from[c])
            def _(c=c):
                pltpu.make_async_copy(sb.at[:, 1], sb.at[:, c], sw_r.at[c // 2]).wait()

    def backward_zero():
        own = dot_nt(take, sb[1, 1])
        backward(
            HALO, kv0[0], kv0[1], qa0[0], qa0[1], own[HALO : HALO + 1, :], own[8 + HALO : 9 + HALO, :]
        )

    for r in (0, 2):
        sy_copy(r).start()
    sw_send(1)
    add_mate(1)
    add_mate(2)
    relay_qa(2)
    backward_zero()
    add_mate(3)
    relay_qa(3)
    add_x1(0)
    relay_stats()
    relay_qa(4)
    add_x1(1)
    add_x1(2)
    add_x2(0)
    add_x1(3)
    add_x2(1)
    add_x2(2)
    add_x2(3)
    wait_stats()
    trow[...] = dot_nt(take, sb[...].reshape(KEYS, HD))

    def backward_step(s, carry):
        w_wait(qa, wq_s, wq_r, s)
        backward(
            s, kv[s, 0, 1, 1], kv[s, 1, 1, 1], qa[s, 0].reshape(KEYS, HD), qa[s, 1].reshape(KEYS, HD),
            trow[pl.ds(s, 1), :] - bias_row(s, True), trow[pl.ds(s + 8, 1), :],
        )
        hooked(s, AFTER_BACKWARD)
        return carry

    AFTER_BACKWARD = {
        0: [(wait_y, 0), (wait_y, 1), (add_y, 0), (add_y, 1), (send_z, 0)],
        1: [(wait_y, 2), (wait_y, 3), (add_y, 2), (send_z, 1)],
    }
    lax.fori_loop(0, HALO, backward_step, 0)

    def place_outputs():
        for h in range(HEADS):
            cols = slice(h * HD, (h + 1) * HD)
            for n in range(3):
                grads_out[n, :, cols] = head_value(lambda s: res[n, s], h)

    def left(ref, sem):
        pltpu.make_async_copy(ref, ref, sem).wait()

    def wait_sent():
        for buf, y_send, w_sent in ((kv, yk_s, wk_s), (qa, yq_s, wq_s)):
            for r in (0, 2):
                left(buf.at[:, :, r, 1], y_send.at[r // 2])
            for c in ANY_COLS:
                @pl.when(sends_to[c])
                def _(c=c, buf=buf, w_sent=w_sent):
                    left(buf.at[:, :, :, c], w_sent.at[c // 2])
        left(sb.at[0, 0:2], sy_s.at[0])
        for c in ANY_COLS:
            @pl.when(sends_to[c])
            def _(c=c):
                left(sb.at[:, c], sw_s.at[c // 2])
        left(rbuf, dd_s.at[0])
        left(x1buf, x1_s.at[0])
        left(x2buf, x2_s.at[0])
        left(ybuf, yy_s.at[0])

    def flush():
        @pl.when(own_z)
        def _():
            left(zr.at[0:7], zz_s.at[0])

        @pl.when(jnp.logical_not(own_z))
        def _():
            left(zr, zz_s.at[0])

    place_outputs()
    wait_sent()
    add_z()
    flush()


def put_out(grads, gw, gq_out, gk_out, gv_out, gw_out, sem):
    copies = [
        pltpu.make_async_copy(grads.at[n], ref, sem.at[n]) for n, ref in enumerate((gq_out, gk_out, gv_out))
    ]
    copies.append(pltpu.make_async_copy(gw, gw_out, sem.at[3]))
    for copy in copies:
        copy.start()
    for copy in copies:
        copy.wait()


def shards(queries, key_tiles, value_tiles, out_grad, w_out, reaches):
    dma = pltpu.SemaphoreType.DMA
    vm = pltpu.VMEM
    shapes = [
        pltpu.SMEM((HEADS, 6), jnp.int32),
        vm((TILE, HQ), BF), vm((TILE, HQ), BF), vm((TILE, HQ), BF), vm((TILE, D), BF), vm((D, HQ), BF),
        vm((TILE, HQ), BF), vm((D, TILE), BF),
        vm((HALO, 2, 3, 3, TILE, HD), BF), vm((HALO, 2, 3, 3, TILE, HD), BF),
        vm((2, TILE, HD), BF), vm((2, TILE, HD), BF),
        vm((TILE, HD), F32), vm((3, 3, TILE, HD), BF), vm((16, KEYS), F32),
        vm((TILE, KEYS), F32), vm((TILE, KEYS), F32), vm((TILE, KEYS), BF), vm((TILE, KEYS), BF),
        vm((2, TILE, HD), BF), vm((3, HEADS, TILE, HD), BF),
        vm((6, 2, 4, 192, HD), BF), vm((6, 4, 192, HD), BF), vm((6, 4, 192, HD), BF),
        vm((2, 6, 192, HD), BF), vm((6, 192, HD), BF), vm((6, 192, HD), BF),
        vm((6, 4, 48, HD), BF), vm((3, 6, 48, HD), BF),
        vm((8, 3, 16, HD), BF), vm((8, 3, 16, HD), BF), vm((6, 8, HD), F32),
        dma((6,)),
    ]
    for sends, receives in (
        ((2,), (HALO, 2)), ((2,), (HALO, 2)), ((2,), (HALO, 2)), ((2,), (HALO, 2)), ((1,), (2,)), ((2,), (2,)),
        ((1,), (4,)), ((1,), (4, 2)), ((1,), (4,)), ((1,), (4,)), ((1,), (2,)),
    ):
        shapes += [dma(sends), dma(receives)]
    anywhere = pl.BlockSpec(memory_space=pl.ANY)
    inside = pl.BlockSpec(memory_space=pltpu.VMEM)
    grads, gw = pl.pallas_call(
        kernel,
        out_shape=(pltpu.VMEM((3, TILE, HQ), BF), pltpu.VMEM((6, HQ), F32)),
        in_specs=[anywhere] * 6,
        out_specs=(inside,) * 2,
        scratch_shapes=shapes,
        compiler_params=pltpu.CompilerParams(collective_id=0, has_side_effects=True),
    )(
        reaches,
        queries.reshape(TILE, HQ),
        key_tiles.reshape(TILE, HQ),
        value_tiles.reshape(TILE, HQ),
        out_grad.reshape(TILE, D),
        w_out,
    )
    tile = jax.ShapeDtypeStruct((TILE, HQ), BF)
    gq, gk, gv, gw = pl.pallas_call(
        put_out,
        out_shape=(tile, tile, tile, jax.ShapeDtypeStruct((6, HQ), F32)),
        in_specs=[inside] * 2,
        out_specs=(anywhere,) * 4,
        scratch_shapes=[dma((4,))],
    )(*(pltpu.with_memory_space_constraint(value, pltpu.VMEM) for value in (grads, gw)))
    return gq.reshape(queries.shape), gk.reshape(queries.shape), gv.reshape(queries.shape), gw


def solution(mesh):
    tiles = P("dp", None, "ha", "wa", None, None)
    return jax.shard_map(
        shards,
        mesh=mesh,
        in_specs=(tiles, tiles, tiles, tiles, P(), P()),
        out_specs=(tiles, tiles, tiles, P(("dp", "ha", "wa"), None)),
        check_vma=False,
    )
```

```python
import math

import jax
import jax.numpy as jnp
from jax import lax
from jax.experimental import pallas as pl
from jax.experimental.pallas import tpu as pltpu
from jax.sharding import PartitionSpec as P

MESH = pl.DeviceIdType.MESH
HEADS = 6
HALO = 5
HD = 128
TILE = 144
KEYS = 9 * TILE
HQ = HEADS * HD
D = 1536
SCALE = 1.0 / math.sqrt(HD)
ROWS = 16
FORWARD_UNROLL = 9
BF = jnp.bfloat16
F32 = jnp.float32
ANY_COLS = (0, 2)
Z_FIRST = 2


def dot(a, b):
    return jnp.dot(a, b, preferred_element_type=F32)


def dot_nt(a, b):
    return lax.dot_general(a, b, (((1,), (1,)), ((), ())), preferred_element_type=F32)


def kernel(
    reach_in, q_in, k_in, v_in, og_in, w_in,
    grads_out, gw_out,
    reach, q_v, k_v, v_v, og_v, w_v, a_v, ogt, kv, qa, kv0, qa0, stat, sb, trow,
    s_buf, dp_buf, p_buf, ds_buf, att_buf, res,
    gbuf, rbuf, abuf, x1buf, xs, x2buf, cbuf, ybuf, zbuf, zr, gws,
    in_sem, yk_s, yk_r, yq_s, yq_r, wk_s, wk_r, wq_s, wq_r, sy_s, sy_r, sw_s, sw_r,
    dd_s, dd_r, x1_s, x1_r, x2_s, x2_r, yy_s, yy_r, zz_s, zz_r, yc_s, yc_r,
):
    dp = lax.axis_index("dp")
    ha = lax.axis_index("ha")
    wa = lax.axis_index("wa")
    x = lax.rem(dp, 4)
    z_hi = lax.div(dp, 4)
    core = lax.rem(wa, 2)
    z_lo = lax.div(wa, 2)
    zi = z_hi * 4 + z_lo
    mate = wa + 1 - 2 * core
    x_one = x + 1 - 2 * lax.rem(x, 2)
    x_three = 3 - x
    x_far = lax.rem(x + 2, 4)
    x_a = x_one + core * (x_three - x_one)
    x_b = x_three + core * (x_one - x_three)
    has_left = wa > 0
    has_right = wa < 7

    def at(dp_=dp, ha_=ha, wa_=wa):
        return (dp_, ha_, wa_)

    loads = [
        pltpu.make_async_copy(src, dst, in_sem.at[n])
        for n, (src, dst) in enumerate(
            ((k_in, k_v), (v_in, v_v), (q_in, q_v), (og_in, og_v), (w_in, w_v), (reach_in, reach))
        )
    ]
    for n in (5, 0, 1, 3, 4, 2):
        loads[n].start()

    barrier = pltpu.get_barrier_semaphore()

    def greet(device):
        pl.semaphore_signal(barrier, inc=1, device_id=device, device_id_type=MESH)

    for dy in (1, 2, 3):
        greet(at(ha_=lax.rem(ha + dy, 4)))
    greet(at(wa_=mate))
    greet(at(dp_=z_hi * 4 + x_one))
    greet(at(dp_=z_hi * 4 + x_three))

    def z_target(shift, other):
        zl = lax.rem(z_lo + shift, 4)
        to_core = 1 - core if other else core
        return at(dp_=core * 4 + x, wa_=zl * 2 + to_core)

    for dz in range(1, 8):
        zt = lax.rem(zi + dz, 8)
        greet(at(dp_=lax.div(zt, 4) * 4 + x, wa_=lax.rem(zt, 4) * 2 + z_hi))
    own_z = z_hi == core
    far_right = (core == 1) & has_right
    far_left = (core == 0) & has_left

    @pl.when(far_right)
    def _():
        greet(at(wa_=wa + 1))

    @pl.when(far_left)
    def _():
        greet(at(wa_=wa - 1))

    def columns(ref, head):
        return ref[:, head * HD : (head + 1) * HD]

    def slot_columns(ref, slot):
        return jnp.where(slot >= zero_head, columns(ref, slot + 1), columns(ref, slot))

    def zero_columns(ref):
        value = columns(ref, 0)
        for h in range(1, HEADS):
            value = jnp.where(zero_head == h, columns(ref, h), value)
        return value

    def head_value(of_slot, h):
        value = jnp.where(zero_head == h, of_slot(HALO), of_slot(min(h, HALO - 1)))
        return jnp.where(zero_head < h, of_slot(h - 1), value) if h else value

    @pl.when(wa == 0)
    def _():
        for buf in (kv, qa):
            def clear(s, carry, buf=buf):
                for kind in range(2):
                    for r in range(3):
                        buf[s, kind, r, 0] = jnp.zeros((TILE, HD), BF)
                return carry
            lax.fori_loop(0, HALO, clear, 0)
        for r in range(3):
            sb[r, 0] = jnp.zeros((TILE, HD), BF)

    @pl.when(wa == 7)
    def _():
        for buf in (kv, qa):
            def clear(s, carry, buf=buf):
                for kind in range(2):
                    for r in range(3):
                        buf[s, kind, r, 2] = jnp.zeros((TILE, HD), BF)
                return carry
            lax.fori_loop(0, HALO, clear, 0)
        for r in range(3):
            sb[r, 2] = jnp.zeros((TILE, HD), BF)

    loads[5].wait()

    zero_head = jnp.int32(0)
    for n in reversed(range(HEADS)):
        total = reach[n, 0]
        for t in range(1, 6):
            total = total + reach[n, t]
        zero_head = jnp.where(total == 0, n, zero_head)

    loads[0].wait()
    loads[1].wait()

    def place_own_kv():
        for s in range(HALO):
            kv[s, 0, 1, 1] = slot_columns(k_v, s)
            kv[s, 1, 1, 1] = slot_columns(v_v, s)
        kv0[0] = zero_columns(k_v)
        kv0[1] = zero_columns(v_v)

    place_own_kv()

    ha_up = lax.rem(ha + 3, 4)
    ha_down = lax.rem(ha + 1, 4)
    wa_right = jnp.minimum(wa + 1, 7)
    wa_left = jnp.maximum(wa - 1, 0)

    def y_copy(buf, send, recv, s, r):
        return pltpu.make_async_remote_copy(
            src_ref=buf.at[s, :, 1, 1], dst_ref=buf.at[s, :, r, 1],
            send_sem=send.at[r // 2], recv_sem=recv.at[s, r // 2],
            device_id=at(ha_=ha_up if r == 2 else ha_down), device_id_type=MESH,
        )

    def w_copy(buf, send, recv, s, r, c):
        return pltpu.make_async_remote_copy(
            src_ref=buf.at[s, :, r, 1], dst_ref=buf.at[s, :, r, c],
            send_sem=send.at[c // 2], recv_sem=recv.at[s, c // 2],
            device_id=at(wa_=wa_right if c == 0 else wa_left), device_id_type=MESH,
        )

    sends_to = {0: has_right, 2: has_left}
    gets_from = {0: has_left, 2: has_right}

    def w_send(buf, send, recv, s, r):
        for c in ANY_COLS:
            @pl.when(sends_to[c])
            def _(c=c):
                w_copy(buf, send, recv, s, r, c).start()

    def relay(buf, y_send, y_recv, w_s, w_r, s):
        for r in (0, 2):
            y_copy(buf, y_send, y_recv, s, r).wait_recv()
            w_send(buf, w_s, w_r, s, r)

    def w_wait(buf, send, recv, s):
        for c in ANY_COLS:
            @pl.when(gets_from[c])
            def _(c=c):
                pltpu.make_async_copy(buf.at[s, :, :, 1], buf.at[s, :, :, c], recv.at[s, c // 2]).wait()

    def relay_kv(s):
        relay(kv, yk_s, yk_r, wk_s, wk_r, s)

    off_chip = {0: core == 0, 2: core == 1}
    leaves_chip = {0: core == 1, 2: core == 0}

    def relay_qa(s):
        if s < Z_FIRST:
            relay(qa, yq_s, yq_r, wq_s, wq_r, s)
            return
        for r in (0, 2):
            y_copy(qa, yq_s, yq_r, s, r).wait_recv()
            for c in ANY_COLS:
                @pl.when(jnp.logical_not(leaves_chip[c]))
                def _(c=c, r=r):
                    w_copy(qa, wq_s, wq_r, s, r, c).start()

    def corner_copy(s, r, c):
        return pltpu.make_async_remote_copy(
            src_ref=qa.at[s, :, 1, c], dst_ref=qa.at[s, :, r, c],
            send_sem=yc_s.at[r // 2], recv_sem=yc_r.at[s - Z_FIRST, r // 2],
            device_id=at(ha_=ha_up if r == 2 else ha_down), device_id_type=MESH,
        )

    def relay_corner(s):
        for c in ANY_COLS:
            @pl.when(gets_from[c] & off_chip[c])
            def _(c=c):
                w_copy(qa, wq_s, wq_r, s, 1, c).wait_recv()
                for r in (0, 2):
                    corner_copy(s, r, c).start()

    def wait_qa(s):
        @pl.when(s < Z_FIRST)
        def _():
            w_wait(qa, wq_s, wq_r, s)

        @pl.when(s >= Z_FIRST)
        def _():
            for c in ANY_COLS:
                @pl.when(jnp.logical_not(off_chip[c]))
                def _(c=c):
                    pltpu.make_async_copy(qa.at[s, :, :, 1], qa.at[s, :, :, c], wq_r.at[s, c // 2]).wait()

                @pl.when(gets_from[c] & off_chip[c])
                def _(c=c):
                    for r in (0, 2):
                        corner_copy(s, r, c).wait_recv()

    def wait_barrier():
        pl.semaphore_wait(barrier, 14 - 2 * own_z.astype(jnp.int32) + (far_right | far_left).astype(jnp.int32))

    wait_barrier()

    def first_kv(s, carry):
        for r in (0, 2):
            y_copy(kv, yk_s, yk_r, s, r).start()
        w_send(kv, wk_s, wk_r, s, 1)
        return carry

    lax.fori_loop(0, HALO, first_kv, 0)

    def wait_loads():
        loads[2].wait()
        loads[3].wait()
        loads[4].wait()

    def amat():
        a_v[...] = dot(og_v[...], w_v[...]).astype(BF)

    def place_own_qa():
        for s in range(HALO):
            qa[s, 0, 1, 1] = slot_columns(q_v, s)
            qa[s, 1, 1, 1] = slot_columns(a_v, s)
            for r in (0, 2):
                y_copy(qa, yq_s, yq_r, s, r).start()
        qa0[0] = zero_columns(q_v)
        qa0[1] = zero_columns(a_v)

    eye = (
        lax.broadcasted_iota(jnp.int32, (HD, HD), 0) == lax.broadcasted_iota(jnp.int32, (HD, HD), 1)
    ).astype(F32).astype(BF)

    def transpose_og():
        for t in range(D // HD):
            ogt[t * HD : (t + 1) * HD, :] = dot_nt(eye, og_v[:, t * HD : (t + 1) * HD]).astype(BF)

    wait_loads()
    amat()
    place_own_qa()
    transpose_og()

    stat[...] = jnp.zeros((TILE, HD), F32)
    lane = lax.broadcasted_iota(jnp.int32, (ROWS, HD), 1)
    key_id = lax.broadcasted_iota(jnp.int32, (1, KEYS), 1)
    place = jnp.zeros((1, KEYS), jnp.int32)
    for n in range(1, 9):
        place = place + (key_id >= n * TILE).astype(jnp.int32)
    row_id = (key_id >= 3 * TILE).astype(jnp.int32) + (key_id >= 6 * TILE).astype(jnp.int32)
    col_id = place - 3 * row_id

    def bias_row(s, mirrored):
        later = s >= zero_head
        up, down, left, right = (jnp.where(later, reach[s + 1, t], reach[s, t]) for t in range(2, 6))
        if mirrored:
            up, down, left, right = down, up, right, left

        def bias(ok):
            return jnp.where(ok, 0.0, -jnp.inf).astype(F32)

        b_up = bias((up > 0) & (ha > 0))
        b_down = bias((down > 0) & (ha < 3))
        b_left = bias((left > 0) & has_left)
        b_right = bias((right > 0) & has_right)
        zero = jnp.zeros((1, KEYS), F32)
        by_row = jnp.where(row_id == 0, zero + b_up, jnp.where(row_id == 2, zero + b_down, zero))
        by_col = jnp.where(col_id == 0, zero + b_left, jnp.where(col_id == 2, zero + b_right, zero))
        return by_row + by_col

    def split3(value):
        high = value.astype(BF).astype(F32)
        rest = value - high
        mid = rest.astype(BF).astype(F32)
        return high, mid, rest - mid

    def forward(slot, q, a, k, v, bias):
        n = k.shape[0]
        s_buf[:, :n] = dot_nt(q, k)
        dp_buf[:, :n] = dot_nt(a, v)

        def rows_step(i, carry):
            rows = pl.ds(pl.multiple_of(i * ROWS, ROWS), ROWS)
            s = s_buf[rows, :n] * SCALE
            if bias is not None:
                s = s + bias
            d = dp_buf[rows, :n]
            peak = jnp.max(s, axis=1, keepdims=True)
            e = jnp.exp(s - peak)
            total = jnp.sum(e, axis=1, keepdims=True)
            p = e * (1.0 / total)
            delta = jnp.sum(p * d, axis=1, keepdims=True)
            p_buf[rows, :n] = p.astype(BF)
            ds_buf[rows, :n] = (p * (d - delta)).astype(BF)
            block = stat[rows, :]
            for base, parts in ((0, split3(peak + jnp.log(total))), (64, split3(delta))):
                for t, part in enumerate(parts):
                    block = jnp.where(lane == base + 3 * slot + t, part, block)
            stat[rows, :] = block
            return carry

        lax.fori_loop(0, TILE // ROWS, rows_step, 0, unroll=FORWARD_UNROLL if n == KEYS else True)
        att_buf[lax.rem(slot + 1, 2)] = dot(p_buf[:, :n], v).astype(BF)
        res[0, slot] = (dot(ds_buf[:, :n], k) * SCALE).astype(BF)

    def backward(slot, k, v, q, a, lse_row, delta_row):
        n = q.shape[0]
        s_buf[:, :n] = dot_nt(k, q)
        dp_buf[:, :n] = dot_nt(v, a)

        def rows_step(i, carry):
            rows = pl.ds(pl.multiple_of(i * ROWS, ROWS), ROWS)
            p = jnp.exp(s_buf[rows, :n] * SCALE - lse_row)
            p_buf[rows, :n] = p.astype(BF)
            ds_buf[rows, :n] = (p * (dp_buf[rows, :n] - delta_row)).astype(BF)
            return carry

        lax.fori_loop(0, TILE // ROWS, rows_step, 0)
        res[2, slot] = dot(p_buf[:, :n], a).astype(BF)
        res[1, slot] = (dot(ds_buf[:, :n], q) * SCALE).astype(BF)

    GROUPS = tuple((unit, 1) for unit in range(HEADS))

    def units(group):
        return pl.ds(*GROUPS[group])

    def weight_term(group):
        unit, count = GROUPS[group]
        if count == 2:
            attended = jnp.concatenate([att_buf[0], att_buf[1]], axis=1)
        else:
            attended = att_buf[unit % 2]
        for t in range(8):
            both = dot(ogt[t * 192 : (t + 1) * 192, :], attended).astype(BF)
            for n in range(count):
                gbuf[unit + n, t // 4, t % 4] = both[:, n * HD : (n + 1) * HD]

    def mate_copy(g):
        return pltpu.make_async_remote_copy(
            src_ref=gbuf.at[units(g), 1 - core], dst_ref=rbuf.at[units(g)],
            send_sem=dd_s.at[0], recv_sem=dd_r.at[g], device_id=at(wa_=mate), device_id_type=MESH,
        )

    def x1_copy(g, which):
        return pltpu.make_async_remote_copy(
            src_ref=abuf.at[units(g), x_far if which else x_a], dst_ref=x1buf.at[which, units(g)],
            send_sem=x1_s.at[0], recv_sem=x1_r.at[g, which],
            device_id=at(dp_=z_hi * 4 + x_a), device_id_type=MESH,
        )

    def x2_copy(g):
        return pltpu.make_async_remote_copy(
            src_ref=xs.at[units(g)], dst_ref=x2buf.at[units(g)],
            send_sem=x2_s.at[0], recv_sem=x2_r.at[g],
            device_id=at(dp_=z_hi * 4 + x_b), device_id_type=MESH,
        )

    def y_sum_copy(g, dy):
        to = lax.rem(ha + dy, 4)
        return pltpu.make_async_remote_copy(
            src_ref=cbuf.at[units(g), to], dst_ref=ybuf.at[dy - 1, units(g)],
            send_sem=yy_s.at[0], recv_sem=yy_r.at[g],
            device_id=at(ha_=to), device_id_type=MESH,
        )

    Z_GROUPS = ((0, 2), (2, 1))

    def z_sum_copy(n, shift, other):
        target = lax.rem(z_lo + shift, 4) * 2 + (1 - core if other else core)
        return pltpu.make_async_remote_copy(
            src_ref=zbuf.at[target, pl.ds(*Z_GROUPS[n])],
            dst_ref=zr.at[z_hi * 4 + shift, pl.ds(*Z_GROUPS[n])],
            send_sem=zz_s.at[0], recv_sem=zz_r.at[n],
            device_id=z_target(shift, other), device_id_type=MESH,
        )

    def wide(value):
        return value.astype(F32)

    def unit_range(g):
        return range(GROUPS[g][0], GROUPS[g][0] + GROUPS[g][1])

    def add_mate(g):
        mate_copy(g).wait_recv()

        def add(at_x):
            for u in unit_range(g):
                abuf[u, at_x] = (wide(gbuf[u, core, at_x]) + wide(rbuf[u, at_x])).astype(BF)

        add(x_far)
        x1_copy(g, 1).start()
        add(x_a)
        x1_copy(g, 0).start()
        add(x_b)
        add(x)

    def add_x1(g):
        x1_copy(g, 1).wait_recv()
        for u in unit_range(g):
            xs[u] = (wide(abuf[u, x_b]) + wide(x1buf[1, u])).astype(BF)
        x2_copy(g).start()

    def add_x2(g):
        x1_copy(g, 0).wait_recv()
        x2_copy(g).wait_recv()
        for u in unit_range(g):
            total = wide(abuf[u, x]) + wide(x1buf[0, u]) + wide(x2buf[u])
            cbuf[u] = total.astype(BF).reshape(4, 48, HD)
        for dy in (2, 1, 3):
            y_sum_copy(g, dy).start()

    def wait_y(g):
        pltpu.make_async_copy(ybuf.at[:, units(g)], ybuf.at[:, units(g)], yy_r.at[g]).wait()

    pick = (lax.broadcasted_iota(jnp.int32, (128, 96), 0), lax.broadcasted_iota(jnp.int32, (128, 96), 1))
    spread = (
        ((pick[0] & 7) < 6)
        & (pick[1] == ((pick[0] >> 3) & 1) * 48 + (pick[0] >> 4) * 6 + (pick[0] & 7))
    ).astype(F32).astype(BF)

    def add_y(pair):
        halves = []
        for u in (2 * pair, 2 * pair + 1):
            total = wide(cbuf[u, ha])
            for n in range(3):
                total = total + wide(ybuf[n, u])
            halves.append(total.astype(BF))
        rows = dot(spread, jnp.concatenate(halves, axis=0))
        zbuf[:, pair] = rows.astype(BF).reshape(8, 16, HD)

    def send_z(n):
        for shift in (2, 1, 3, 0):
            z_sum_copy(n, shift, True).start()
            if shift:
                z_sum_copy(n, shift, False).start()

        @pl.when(jnp.logical_not(own_z))
        def _():
            z_sum_copy(n, 0, False).start()

        @pl.when(own_z)
        def _():
            pairs = range(Z_GROUPS[n][0], Z_GROUPS[n][0] + Z_GROUPS[n][1])
            for pair in pairs:
                zr[zi - z_lo, pair] = zbuf[z_lo * 2 + core, pair]

    def z_bytes(ref, count, n):
        part = ref.at[0:count, pl.ds(*Z_GROUPS[n])]
        return part, part

    def add_z():
        for n in range(2):
            @pl.when(own_z)
            def _(n=n):
                pltpu.make_async_copy(*z_bytes(zr, 7, n), zz_r.at[n]).wait()

            @pl.when(jnp.logical_not(own_z))
            def _(n=n):
                pltpu.make_async_copy(*z_bytes(zr, 8, n), zz_r.at[n]).wait()
        for pair in range(3):
            total = wide(zr[0, pair])
            for n in range(1, 8):
                total = total + wide(zr[n, pair])
            gws[2 * pair] = total[:8]
            gws[2 * pair + 1] = total[8:]
        for h in range(HEADS):
            gw_out[:, h * HD : (h + 1) * HD] = head_value(lambda s: gws[(s + 1) % HEADS, 0:6, :], h)

    def own_qa():
        for s in (2, 3, 4, 0, 1):
            w_send(qa, wq_s, wq_r, s, 1)

    def hooked(s, hooks):
        for n, ops in hooks.items():
            @pl.when(s == n)
            def _(ops=ops):
                for op, *args in ops:
                    op(*args)

    def group_done(g):
        weight_term(g)
        mate_copy(g).start()

    forward(HALO, qa0[0], qa0[1], kv0[0], kv0[1], None)
    group_done(0)
    relay_kv(0)
    relay_kv(1)

    def forward_step(s, carry):
        hooked(s, BEFORE_FORWARD)
        w_wait(kv, wk_s, wk_r, s)
        forward(
            s, qa[s, 0, 1, 1], qa[s, 1, 1, 1],
            kv[s, 0].reshape(KEYS, HD), kv[s, 1].reshape(KEYS, HD), bias_row(s, False),
        )
        hooked(s, AFTER_FORWARD)
        return carry

    BEFORE_FORWARD = {
        0: [(relay_kv, 2)],
        1: [(relay_kv, 3)],
        2: [(relay_kv, 4), (own_qa,)],
        3: [(relay_qa, 0)],
        4: [(relay_qa, 1)],
    }
    AFTER_FORWARD = {
        0: [(group_done, 1), (add_mate, 0)],
        1: [(group_done, 2), (add_mate, 1)],
        2: [(group_done, 3), (add_mate, 2), (add_x1, 0)],
        3: [(group_done, 4), (add_mate, 3), (add_x1, 1)],
        4: [(group_done, 5), (add_mate, 4), (add_x1, 2), (add_x2, 0)],
    }
    lax.fori_loop(0, HALO, forward_step, 0)

    sb[1, 1] = stat[...].astype(BF)

    def sy_copy(r):
        return pltpu.make_async_remote_copy(
            src_ref=sb.at[1, 1], dst_ref=sb.at[r, 1], send_sem=sy_s.at[0], recv_sem=sy_r.at[r // 2],
            device_id=at(ha_=ha_up if r == 2 else ha_down), device_id_type=MESH,
        )

    def sw_copy(r, c):
        return pltpu.make_async_remote_copy(
            src_ref=sb.at[r, 1], dst_ref=sb.at[r, c],
            send_sem=sw_s.at[c // 2], recv_sem=sw_r.at[c // 2],
            device_id=at(wa_=wa_right if c == 0 else wa_left), device_id_type=MESH,
        )

    def sw_send(r):
        for c in ANY_COLS:
            @pl.when(sends_to[c])
            def _(c=c):
                sw_copy(r, c).start()

    chosen = (lax.broadcasted_iota(jnp.int32, (16, HD), 0), lax.broadcasted_iota(jnp.int32, (16, HD), 1))
    first = (chosen[0] & 7) * 3 + (chosen[0] >> 3) * 64
    take = ((chosen[1] >= first) & (chosen[1] < first + 3) & ((chosen[0] & 7) < 6)).astype(F32).astype(BF)

    def relay_stats():
        for r in (0, 2):
            sy_copy(r).wait_recv()
            sw_send(r)

    def wait_stats():
        for c in ANY_COLS:
            @pl.when(gets_from[c])
            def _(c=c):
                pltpu.make_async_copy(sb.at[:, 1], sb.at[:, c], sw_r.at[c // 2]).wait()

    def backward_zero():
        own = dot_nt(take, sb[1, 1])
        backward(
            HALO, kv0[0], kv0[1], qa0[0], qa0[1], own[HALO : HALO + 1, :], own[8 + HALO : 9 + HALO, :]
        )

    for r in (0, 2):
        sy_copy(r).start()
    sw_send(1)
    relay_corner(2)
    relay_corner(3)
    relay_corner(4)
    relay_qa(2)
    backward_zero()
    add_mate(5)
    add_x1(3)
    relay_qa(3)
    add_x2(1)
    relay_stats()
    add_x1(4)
    relay_qa(4)
    add_x2(2)
    add_x1(5)
    add_x2(3)
    wait_stats()
    trow[...] = dot_nt(take, sb[...].reshape(KEYS, HD))

    def backward_step(s, carry):
        wait_qa(s)
        backward(
            s, kv[s, 0, 1, 1], kv[s, 1, 1, 1], qa[s, 0].reshape(KEYS, HD), qa[s, 1].reshape(KEYS, HD),
            trow[pl.ds(s, 1), :] - bias_row(s, True), trow[pl.ds(s + 8, 1), :],
        )
        hooked(s, AFTER_BACKWARD)
        return carry

    AFTER_BACKWARD = {
        0: [
            (add_x2, 4), (add_x2, 5), (wait_y, 0), (wait_y, 1), (wait_y, 2), (wait_y, 3),
            (add_y, 0), (add_y, 1), (send_z, 0),
        ],
        2: [(wait_y, 4), (wait_y, 5), (add_y, 2), (send_z, 1)],
    }
    lax.fori_loop(0, HALO, backward_step, 0)

    def place_outputs():
        for h in range(HEADS):
            cols = slice(h * HD, (h + 1) * HD)
            for n in range(3):
                grads_out[n, :, cols] = head_value(lambda s: res[n, s], h)

    def left(ref, sem):
        pltpu.make_async_copy(ref, ref, sem).wait()

    def wait_sent():
        for buf, y_send, w_sent in ((kv, yk_s, wk_s), (qa, yq_s, wq_s)):
            for r in (0, 2):
                left(buf.at[:, :, r, 1], y_send.at[r // 2])
            for c in ANY_COLS:
                if buf is kv:
                    @pl.when(sends_to[c])
                    def _(c=c):
                        left(kv.at[:, :, :, c], wk_s.at[c // 2])
                    continue

                @pl.when(jnp.logical_not(leaves_chip[c]))
                def _(c=c):
                    left(qa.at[:, :, :, c], wq_s.at[c // 2])

                @pl.when(sends_to[c] & leaves_chip[c])
                def _(c=c):
                    left(qa.at[0], wq_s.at[c // 2])
        for c in ANY_COLS:
            @pl.when(gets_from[c] & off_chip[c])
            def _(c=c):
                for r in (0, 2):
                    left(qa.at[0, 0, 0:2], yc_s.at[r // 2])
        left(sb.at[0, 0:2], sy_s.at[0])
        for c in ANY_COLS:
            @pl.when(sends_to[c])
            def _(c=c):
                left(sb.at[:, c], sw_s.at[c // 2])
        left(rbuf, dd_s.at[0])
        left(x1buf, x1_s.at[0])
        left(x2buf, x2_s.at[0])
        left(ybuf, yy_s.at[0])

    def flush():
        @pl.when(own_z)
        def _():
            left(zr.at[0:7], zz_s.at[0])

        @pl.when(jnp.logical_not(own_z))
        def _():
            left(zr, zz_s.at[0])

    place_outputs()
    wait_sent()
    add_z()
    flush()


def put_out(grads, gw, gq_out, gk_out, gv_out, gw_out, sem):
    copies = [
        pltpu.make_async_copy(grads.at[n], ref, sem.at[n]) for n, ref in enumerate((gq_out, gk_out, gv_out))
    ]
    copies.append(pltpu.make_async_copy(gw, gw_out, sem.at[3]))
    for copy in copies:
        copy.start()
    for copy in copies:
        copy.wait()


def shards(queries, key_tiles, value_tiles, out_grad, w_out, reaches):
    dma = pltpu.SemaphoreType.DMA
    vm = pltpu.VMEM
    shapes = [
        pltpu.SMEM((HEADS, 6), jnp.int32),
        vm((TILE, HQ), BF), vm((TILE, HQ), BF), vm((TILE, HQ), BF), vm((TILE, D), BF), vm((D, HQ), BF),
        vm((TILE, HQ), BF), vm((D, TILE), BF),
        vm((HALO, 2, 3, 3, TILE, HD), BF), vm((HALO, 2, 3, 3, TILE, HD), BF),
        vm((2, TILE, HD), BF), vm((2, TILE, HD), BF),
        vm((TILE, HD), F32), vm((3, 3, TILE, HD), BF), vm((16, KEYS), F32),
        vm((TILE, KEYS), F32), vm((TILE, KEYS), F32), vm((TILE, KEYS), BF), vm((TILE, KEYS), BF),
        vm((2, TILE, HD), BF), vm((3, HEADS, TILE, HD), BF),
        vm((6, 2, 4, 192, HD), BF), vm((6, 4, 192, HD), BF), vm((6, 4, 192, HD), BF),
        vm((2, 6, 192, HD), BF), vm((6, 192, HD), BF), vm((6, 192, HD), BF),
        vm((6, 4, 48, HD), BF), vm((3, 6, 48, HD), BF),
        vm((8, 3, 16, HD), BF), vm((8, 3, 16, HD), BF), vm((6, 8, HD), F32),
        dma((6,)),
    ]
    for sends, receives in (
        ((2,), (HALO, 2)), ((2,), (HALO, 2)), ((2,), (HALO, 2)), ((2,), (HALO, 2)), ((1,), (2,)), ((2,), (2,)),
        ((1,), (6,)), ((1,), (6, 2)), ((1,), (6,)), ((1,), (6,)), ((1,), (2,)), ((2,), (HALO - Z_FIRST, 2)),
    ):
        shapes += [dma(sends), dma(receives)]
    anywhere = pl.BlockSpec(memory_space=pl.ANY)
    inside = pl.BlockSpec(memory_space=pltpu.VMEM)
    grads, gw = pl.pallas_call(
        kernel,
        out_shape=(pltpu.VMEM((3, TILE, HQ), BF), pltpu.VMEM((6, HQ), F32)),
        in_specs=[anywhere] * 6,
        out_specs=(inside,) * 2,
        scratch_shapes=shapes,
        compiler_params=pltpu.CompilerParams(collective_id=0, has_side_effects=True),
    )(
        reaches,
        queries.reshape(TILE, HQ),
        key_tiles.reshape(TILE, HQ),
        value_tiles.reshape(TILE, HQ),
        out_grad.reshape(TILE, D),
        w_out,
    )
    tile = jax.ShapeDtypeStruct((TILE, HQ), BF)
    gq, gk, gv, gw = pl.pallas_call(
        put_out,
        out_shape=(tile, tile, tile, jax.ShapeDtypeStruct((6, HQ), F32)),
        in_specs=[inside] * 2,
        out_specs=(anywhere,) * 4,
        scratch_shapes=[dma((4,))],
    )(*(pltpu.with_memory_space_constraint(value, pltpu.VMEM) for value in (grads, gw)))
    return gq.reshape(queries.shape), gk.reshape(queries.shape), gv.reshape(queries.shape), gw


def solution(mesh):
    tiles = P("dp", None, "ha", "wa", None, None)
    return jax.shard_map(
        shards,
        mesh=mesh,
        in_specs=(tiles, tiles, tiles, tiles, P(), P()),
        out_specs=(tiles, tiles, tiles, P(("dp", "ha", "wa"), None)),
        check_vma=False,
    )
```

```python
import math

import jax
import jax.numpy as jnp
from jax import lax
from jax.experimental import pallas as pl
from jax.experimental.pallas import tpu as pltpu
from jax.sharding import PartitionSpec as P

MESH = pl.DeviceIdType.MESH
HEADS = 6
HALO = 5
HD = 128
TILE = 144
KEYS = 9 * TILE
HQ = HEADS * HD
D = 1536
SCALE = 1.0 / math.sqrt(HD)
LOG2E = 1.0 / math.log(2.0)
SCALE2 = SCALE * LOG2E
ROWS = 16
FORWARD_UNROLL = 9
BF = jnp.bfloat16
F32 = jnp.float32
ANY_COLS = (0, 2)
DIRECT = 4
Z_FIRST = 3


def dot(a, b):
    return jnp.dot(a, b, preferred_element_type=F32)


def dot_nt(a, b):
    return lax.dot_general(a, b, (((1,), (1,)), ((), ())), preferred_element_type=F32)


def kernel(
    reach_in, q_in, k_in, v_in, og_in, w_in,
    grads_out, gw_out,
    reach, q_v, k_v, v_v, og_v, w_v, a_v, ogt, kv, qa, kv0, qa0, stat, sb, trow,
    s_buf, dp_buf, p_buf, ds_buf, att_buf, res,
    gbuf, rbuf, abuf, x1buf, xs, x2buf, cbuf, ybuf, xbuf, yxbuf, zbuf, zr, gws,
    in_sem, yk_s, yk_r, yq_s, yq_r, wk_s, wk_r, wq_s, wq_r, sy_s, sy_r, sw_s, sw_r,
    dd_s, dd_r, x1_s, x1_r, x2_s, x2_r, yy_s, yy_r, zz_s, zz_r, yc_s, yc_r, yx_s, yx_r, zq_s,
):
    dp = lax.axis_index("dp")
    ha = lax.axis_index("ha")
    wa = lax.axis_index("wa")
    x = lax.rem(dp, 4)
    z_hi = lax.div(dp, 4)
    core = lax.rem(wa, 2)
    z_lo = lax.div(wa, 2)
    zi = z_hi * 4 + z_lo
    mate = wa + 1 - 2 * core
    x_one = x + 1 - 2 * lax.rem(x, 2)
    x_three = 3 - x
    x_far = lax.rem(x + 2, 4)
    x_a = x_one + core * (x_three - x_one)
    x_b = x_three + core * (x_one - x_three)
    has_left = wa > 0
    has_right = wa < 7

    def at(dp_=dp, ha_=ha, wa_=wa):
        return (dp_, ha_, wa_)

    loads = [
        pltpu.make_async_copy(src, dst, in_sem.at[n])
        for n, (src, dst) in enumerate(
            ((k_in, k_v), (v_in, v_v), (q_in, q_v), (og_in, og_v), (w_in, w_v), (reach_in, reach))
        )
    ]
    for n in (5, 0, 1, 3, 4, 2):
        loads[n].start()

    barrier = pltpu.get_barrier_semaphore()

    def greet(device):
        pl.semaphore_signal(barrier, inc=1, device_id=device, device_id_type=MESH)

    for dy in (1, 2, 3):
        greet(at(ha_=lax.rem(ha + dy, 4)))
        greet(at(dp_=z_hi * 4 + x_b, ha_=lax.rem(ha + dy, 4)))
    greet(at(wa_=mate))
    greet(at(dp_=z_hi * 4 + x_one))
    greet(at(dp_=z_hi * 4 + x_three))

    def z_target(shift, other):
        zl = lax.rem(z_lo + shift, 4)
        to_core = 1 - core if other else core
        return at(dp_=core * 4 + x, wa_=zl * 2 + to_core)

    for dz in range(1, 8):
        zt = lax.rem(zi + dz, 8)
        greet(at(dp_=lax.div(zt, 4) * 4 + x, wa_=lax.rem(zt, 4) * 2 + z_hi))
    own_z = z_hi == core
    far_right = (core == 1) & has_right
    far_left = (core == 0) & has_left

    @pl.when(far_right)
    def _():
        greet(at(wa_=wa + 1))

    @pl.when(far_left)
    def _():
        greet(at(wa_=wa - 1))

    def columns(ref, head):
        return ref[:, head * HD : (head + 1) * HD]

    def slot_columns(ref, slot):
        return jnp.where(slot >= zero_head, columns(ref, slot + 1), columns(ref, slot))

    def zero_columns(ref):
        value = columns(ref, 0)
        for h in range(1, HEADS):
            value = jnp.where(zero_head == h, columns(ref, h), value)
        return value

    def head_value(of_slot, h):
        value = jnp.where(zero_head == h, of_slot(HALO), of_slot(min(h, HALO - 1)))
        return jnp.where(zero_head < h, of_slot(h - 1), value) if h else value

    @pl.when(wa == 0)
    def _():
        for buf in (kv, qa):
            def clear(s, carry, buf=buf):
                for kind in range(2):
                    for r in range(3):
                        buf[s, kind, r, 0] = jnp.zeros((TILE, HD), BF)
                return carry
            lax.fori_loop(0, HALO, clear, 0)
        for r in range(3):
            sb[r, 0] = jnp.zeros((TILE, HD), BF)

    @pl.when(wa == 7)
    def _():
        for buf in (kv, qa):
            def clear(s, carry, buf=buf):
                for kind in range(2):
                    for r in range(3):
                        buf[s, kind, r, 2] = jnp.zeros((TILE, HD), BF)
                return carry
            lax.fori_loop(0, HALO, clear, 0)
        for r in range(3):
            sb[r, 2] = jnp.zeros((TILE, HD), BF)

    loads[5].wait()

    zero_head = jnp.int32(0)
    for n in reversed(range(HEADS)):
        total = reach[n, 0]
        for t in range(1, 6):
            total = total + reach[n, t]
        zero_head = jnp.where(total == 0, n, zero_head)

    loads[0].wait()
    loads[1].wait()

    def place_own_kv():
        for s in range(HALO):
            kv[s, 0, 1, 1] = slot_columns(k_v, s)
            kv[s, 1, 1, 1] = slot_columns(v_v, s)
        kv0[0] = zero_columns(k_v)
        kv0[1] = zero_columns(v_v)

    place_own_kv()

    ha_up = lax.rem(ha + 3, 4)
    ha_down = lax.rem(ha + 1, 4)
    wa_right = jnp.minimum(wa + 1, 7)
    wa_left = jnp.maximum(wa - 1, 0)

    def y_copy(buf, send, recv, s, r):
        return pltpu.make_async_remote_copy(
            src_ref=buf.at[s, :, 1, 1], dst_ref=buf.at[s, :, r, 1],
            send_sem=send.at[r // 2], recv_sem=recv.at[s, r // 2],
            device_id=at(ha_=ha_up if r == 2 else ha_down), device_id_type=MESH,
        )

    def w_copy(buf, send, recv, s, r, c):
        return pltpu.make_async_remote_copy(
            src_ref=buf.at[s, :, r, 1], dst_ref=buf.at[s, :, r, c],
            send_sem=send.at[c // 2], recv_sem=recv.at[s, c // 2],
            device_id=at(wa_=wa_right if c == 0 else wa_left), device_id_type=MESH,
        )

    sends_to = {0: has_right, 2: has_left}
    gets_from = {0: has_left, 2: has_right}

    def w_send(buf, send, recv, s, r):
        for c in ANY_COLS:
            @pl.when(sends_to[c])
            def _(c=c):
                w_copy(buf, send, recv, s, r, c).start()

    def relay(buf, y_send, y_recv, w_s, w_r, s):
        for r in (0, 2):
            y_copy(buf, y_send, y_recv, s, r).wait_recv()
            w_send(buf, w_s, w_r, s, r)

    def w_wait(buf, send, recv, s):
        for c in ANY_COLS:
            @pl.when(gets_from[c])
            def _(c=c):
                pltpu.make_async_copy(buf.at[s, :, :, 1], buf.at[s, :, :, c], recv.at[s, c // 2]).wait()

    def relay_kv(s):
        relay(kv, yk_s, yk_r, wk_s, wk_r, s)

    off_chip = {0: core == 0, 2: core == 1}
    leaves_chip = {0: core == 1, 2: core == 0}

    def relay_qa(s):
        if s < Z_FIRST:
            relay(qa, yq_s, yq_r, wq_s, wq_r, s)
            return
        for r in (0, 2):
            y_copy(qa, yq_s, yq_r, s, r).wait_recv()
            for c in ANY_COLS:
                @pl.when(jnp.logical_not(leaves_chip[c]))
                def _(c=c, r=r):
                    w_copy(qa, wq_s, wq_r, s, r, c).start()

    def corner_copy(s, r, c):
        return pltpu.make_async_remote_copy(
            src_ref=qa.at[s, :, 1, c], dst_ref=qa.at[s, :, r, c],
            send_sem=yc_s.at[r // 2], recv_sem=yc_r.at[s - Z_FIRST, r // 2],
            device_id=at(ha_=ha_up if r == 2 else ha_down), device_id_type=MESH,
        )

    def z_first_copy(s, c):
        return pltpu.make_async_remote_copy(
            src_ref=qa.at[s, :, 1, 1], dst_ref=qa.at[s, :, 1, c],
            send_sem=zq_s.at[0], recv_sem=wq_r.at[s, c // 2],
            device_id=at(wa_=wa_right if c == 0 else wa_left), device_id_type=MESH,
        )

    def relay_corner(s):
        for c in ANY_COLS:
            @pl.when(gets_from[c] & off_chip[c])
            def _(c=c):
                w_copy(qa, wq_s, wq_r, s, 1, c).wait_recv()
                for r in (0, 2):
                    corner_copy(s, r, c).start()

    def wait_qa(s):
        @pl.when(s < Z_FIRST)
        def _():
            w_wait(qa, wq_s, wq_r, s)

        @pl.when(s >= Z_FIRST)
        def _():
            for c in ANY_COLS:
                @pl.when(jnp.logical_not(off_chip[c]))
                def _(c=c):
                    pltpu.make_async_copy(qa.at[s, :, :, 1], qa.at[s, :, :, c], wq_r.at[s, c // 2]).wait()

                @pl.when(gets_from[c] & off_chip[c])
                def _(c=c):
                    for r in (0, 2):
                        corner_copy(s, r, c).wait_recv()

    def wait_barrier():
        pl.semaphore_wait(barrier, 17 - 2 * own_z.astype(jnp.int32) + (far_right | far_left).astype(jnp.int32))

    wait_barrier()

    def first_kv(s, carry):
        for r in (0, 2):
            y_copy(kv, yk_s, yk_r, s, r).start()
        w_send(kv, wk_s, wk_r, s, 1)
        return carry

    lax.fori_loop(0, HALO, first_kv, 0)

    def wait_loads():
        loads[2].wait()
        loads[3].wait()
        loads[4].wait()

    def amat():
        a_v[...] = dot(og_v[...], w_v[...]).astype(BF)

    def place_own_qa():
        for s in range(HALO):
            qa[s, 0, 1, 1] = slot_columns(q_v, s)
            qa[s, 1, 1, 1] = slot_columns(a_v, s)
            for r in (0, 2):
                y_copy(qa, yq_s, yq_r, s, r).start()
        qa0[0] = zero_columns(q_v)
        qa0[1] = zero_columns(a_v)

    eye = (
        lax.broadcasted_iota(jnp.int32, (HD, HD), 0) == lax.broadcasted_iota(jnp.int32, (HD, HD), 1)
    ).astype(F32).astype(BF)

    def transpose_og():
        for t in range(D // HD):
            ogt[t * HD : (t + 1) * HD, :] = dot_nt(eye, og_v[:, t * HD : (t + 1) * HD]).astype(BF)

    wait_loads()
    amat()
    place_own_qa()
    transpose_og()

    stat[...] = jnp.zeros((TILE, HD), F32)
    lane = lax.broadcasted_iota(jnp.int32, (ROWS, HD), 1)
    key_id = lax.broadcasted_iota(jnp.int32, (1, KEYS), 1)
    place = jnp.zeros((1, KEYS), jnp.int32)
    for n in range(1, 9):
        place = place + (key_id >= n * TILE).astype(jnp.int32)
    row_id = (key_id >= 3 * TILE).astype(jnp.int32) + (key_id >= 6 * TILE).astype(jnp.int32)
    col_id = place - 3 * row_id

    def bias_row(s, mirrored):
        later = s >= zero_head
        up, down, left, right = (jnp.where(later, reach[s + 1, t], reach[s, t]) for t in range(2, 6))
        if mirrored:
            up, down, left, right = down, up, right, left

        def bias(ok):
            return jnp.where(ok, 0.0, -jnp.inf).astype(F32)

        b_up = bias((up > 0) & (ha > 0))
        b_down = bias((down > 0) & (ha < 3))
        b_left = bias((left > 0) & has_left)
        b_right = bias((right > 0) & has_right)
        zero = jnp.zeros((1, KEYS), F32)
        by_row = jnp.where(row_id == 0, zero + b_up, jnp.where(row_id == 2, zero + b_down, zero))
        by_col = jnp.where(col_id == 0, zero + b_left, jnp.where(col_id == 2, zero + b_right, zero))
        return by_row + by_col

    def split3(value):
        high = value.astype(BF).astype(F32)
        rest = value - high
        mid = rest.astype(BF).astype(F32)
        return high, mid, rest - mid

    def forward(slot, q, a, k, v, bias):
        n = k.shape[0]
        s_buf[:, :n] = dot_nt(q, k)
        dp_buf[:, :n] = dot_nt(a, v)

        def rows_step(i, carry):
            rows = pl.ds(pl.multiple_of(i * ROWS, ROWS), ROWS)
            s = s_buf[rows, :n] * SCALE2
            if bias is not None:
                s = s + bias
            d = dp_buf[rows, :n]
            peak = jnp.max(s, axis=1, keepdims=True)
            e = jnp.exp2(s - peak)
            total = jnp.sum(e, axis=1, keepdims=True)
            p = e * (1.0 / total)
            delta = jnp.sum(p * d, axis=1, keepdims=True)
            p_buf[rows, :n] = p.astype(BF)
            ds_buf[rows, :n] = (p * (d - delta)).astype(BF)
            block = stat[rows, :]
            for base, parts in ((0, split3(peak + jnp.log(total) * LOG2E)), (64, split3(delta))):
                for t, part in enumerate(parts):
                    block = jnp.where(lane == base + 3 * slot + t, part, block)
            stat[rows, :] = block
            return carry

        lax.fori_loop(0, TILE // ROWS, rows_step, 0, unroll=FORWARD_UNROLL if n == KEYS else True)
        att_buf[lax.rem(slot + 1, 2)] = dot(p_buf[:, :n], v).astype(BF)
        res[0, slot] = (dot(ds_buf[:, :n], k) * SCALE).astype(BF)

    def backward(slot, k, v, q, a, lse_row, delta_row):
        n = q.shape[0]
        s_buf[:, :n] = dot_nt(k, q)
        dp_buf[:, :n] = dot_nt(v, a)

        def rows_step(i, carry):
            rows = pl.ds(pl.multiple_of(i * ROWS, ROWS), ROWS)
            p = jnp.exp2(s_buf[rows, :n] * SCALE2 - lse_row)
            p_buf[rows, :n] = p.astype(BF)
            ds_buf[rows, :n] = (p * (dp_buf[rows, :n] - delta_row)).astype(BF)
            return carry

        lax.fori_loop(0, TILE // ROWS, rows_step, 0)
        res[2, slot] = dot(p_buf[:, :n], a).astype(BF)
        res[1, slot] = (dot(ds_buf[:, :n], q) * SCALE).astype(BF)

    GROUPS = tuple((unit, 1) for unit in range(HEADS))

    def units(group):
        return pl.ds(*GROUPS[group])

    def weight_term(group):
        unit, count = GROUPS[group]
        if count == 2:
            attended = jnp.concatenate([att_buf[0], att_buf[1]], axis=1)
        else:
            attended = att_buf[unit % 2]
        for t in range(8):
            both = dot(ogt[t * 192 : (t + 1) * 192, :], attended).astype(BF)
            for n in range(count):
                gbuf[unit + n, t // 4, t % 4] = both[:, n * HD : (n + 1) * HD]

    def mate_copy(g):
        return pltpu.make_async_remote_copy(
            src_ref=gbuf.at[units(g), 1 - core], dst_ref=rbuf.at[units(g)],
            send_sem=dd_s.at[0], recv_sem=dd_r.at[g], device_id=at(wa_=mate), device_id_type=MESH,
        )

    def x1_copy(g, which):
        return pltpu.make_async_remote_copy(
            src_ref=abuf.at[units(g), x_far if which else x_a], dst_ref=x1buf.at[which, units(g)],
            send_sem=x1_s.at[0], recv_sem=x1_r.at[g, which],
            device_id=at(dp_=z_hi * 4 + x_a), device_id_type=MESH,
        )

    def x2_copy(g):
        return pltpu.make_async_remote_copy(
            src_ref=xs.at[units(g)], dst_ref=x2buf.at[units(g)],
            send_sem=x2_s.at[0], recv_sem=x2_r.at[g],
            device_id=at(dp_=z_hi * 4 + x_b), device_id_type=MESH,
        )

    def y_sum_copy(g, dy):
        to = lax.rem(ha + dy, 4)
        return pltpu.make_async_remote_copy(
            src_ref=cbuf.at[units(g), to], dst_ref=ybuf.at[dy - 1, units(g)],
            send_sem=yy_s.at[0], recv_sem=yy_r.at[g],
            device_id=at(ha_=to), device_id_type=MESH,
        )

    def across_copy(u, dy):
        to = lax.rem(ha + dy, 4)
        return pltpu.make_async_remote_copy(
            src_ref=xbuf.at[u - DIRECT, to], dst_ref=yxbuf.at[dy, u - DIRECT],
            send_sem=yx_s.at[0], recv_sem=yx_r.at[u - DIRECT],
            device_id=at(dp_=z_hi * 4 + x_b, ha_=to), device_id_type=MESH,
        )

    Z_GROUPS = ((0, 2), (2, 1))

    def z_sum_copy(n, shift, other):
        target = lax.rem(z_lo + shift, 4) * 2 + (1 - core if other else core)
        return pltpu.make_async_remote_copy(
            src_ref=zbuf.at[target, pl.ds(*Z_GROUPS[n])],
            dst_ref=zr.at[z_hi * 4 + shift, pl.ds(*Z_GROUPS[n])],
            send_sem=zz_s.at[0], recv_sem=zz_r.at[n],
            device_id=z_target(shift, other), device_id_type=MESH,
        )

    def wide(value):
        return value.astype(F32)

    def unit_range(g):
        return range(GROUPS[g][0], GROUPS[g][0] + GROUPS[g][1])

    def add_mate(g):
        mate_copy(g).wait_recv()

        def add(at_x):
            for u in unit_range(g):
                abuf[u, at_x] = (wide(gbuf[u, core, at_x]) + wide(rbuf[u, at_x])).astype(BF)

        add(x_far)
        x1_copy(g, 1).start()
        add(x_a)
        x1_copy(g, 0).start()
        add(x_b)
        add(x)

    def add_x1(g):
        x1_copy(g, 1).wait_recv()
        for u in unit_range(g):
            xs[u] = (wide(abuf[u, x_b]) + wide(x1buf[1, u])).astype(BF)
        x2_copy(g).start()

    def add_x2(g):
        x1_copy(g, 0).wait_recv()
        x2_copy(g).wait_recv()
        for u in unit_range(g):
            total = wide(abuf[u, x]) + wide(x1buf[0, u]) + wide(x2buf[u])
            cbuf[u] = total.astype(BF).reshape(4, 48, HD)
        for dy in (2, 1, 3):
            y_sum_copy(g, dy).start()

    def wait_y(g):
        pltpu.make_async_copy(ybuf.at[:, units(g)], ybuf.at[:, units(g)], yy_r.at[g]).wait()

    def add_direct(u):
        x1_copy(u, 1).wait_recv()
        total = wide(abuf[u, x_b]) + wide(x1buf[1, u])
        xbuf[u - DIRECT] = total.astype(BF).reshape(4, 48, HD)
        for dy in (2, 1, 3, 0):
            across_copy(u, dy).start()
        x1_copy(u, 0).wait_recv()
        total = wide(abuf[u, x]) + wide(x1buf[0, u])
        cbuf[u] = total.astype(BF).reshape(4, 48, HD)
        for dy in (2, 1, 3):
            y_sum_copy(u, dy).start()

    def wait_direct(u):
        wait_y(u)
        pltpu.make_async_copy(yxbuf.at[:, u - DIRECT], yxbuf.at[:, u - DIRECT], yx_r.at[u - DIRECT]).wait()

    pick = (lax.broadcasted_iota(jnp.int32, (128, 96), 0), lax.broadcasted_iota(jnp.int32, (128, 96), 1))
    spread = (
        ((pick[0] & 7) < 6)
        & (pick[1] == ((pick[0] >> 3) & 1) * 48 + (pick[0] >> 4) * 6 + (pick[0] & 7))
    ).astype(F32).astype(BF)

    def add_y(pair):
        halves = []
        for u in (2 * pair, 2 * pair + 1):
            total = wide(cbuf[u, ha])
            for n in range(3):
                total = total + wide(ybuf[n, u])
            if u >= DIRECT:
                for n in range(4):
                    total = total + wide(yxbuf[n, u - DIRECT])
            halves.append(total.astype(BF))
        rows = dot(spread, jnp.concatenate(halves, axis=0))
        zbuf[:, pair] = rows.astype(BF).reshape(8, 16, HD)

    def send_z(n):
        for shift in (2, 1, 3, 0):
            z_sum_copy(n, shift, True).start()
            if shift:
                z_sum_copy(n, shift, False).start()

        @pl.when(jnp.logical_not(own_z))
        def _():
            z_sum_copy(n, 0, False).start()

        @pl.when(own_z)
        def _():
            pairs = range(Z_GROUPS[n][0], Z_GROUPS[n][0] + Z_GROUPS[n][1])
            for pair in pairs:
                zr[zi - z_lo, pair] = zbuf[z_lo * 2 + core, pair]

    def z_bytes(ref, count, n):
        part = ref.at[0:count, pl.ds(*Z_GROUPS[n])]
        return part, part

    def add_z():
        for n in range(2):
            @pl.when(own_z)
            def _(n=n):
                pltpu.make_async_copy(*z_bytes(zr, 7, n), zz_r.at[n]).wait()

            @pl.when(jnp.logical_not(own_z))
            def _(n=n):
                pltpu.make_async_copy(*z_bytes(zr, 8, n), zz_r.at[n]).wait()
        for pair in range(3):
            total = wide(zr[0, pair])
            for n in range(1, 8):
                total = total + wide(zr[n, pair])
            gws[2 * pair] = total[:8]
            gws[2 * pair + 1] = total[8:]
        for h in range(HEADS):
            gw_out[:, h * HD : (h + 1) * HD] = head_value(lambda s: gws[(s + 1) % HEADS, 0:6, :], h)

    def own_qa():
        for s in range(Z_FIRST, HALO):
            for c in ANY_COLS:
                @pl.when(sends_to[c] & leaves_chip[c])
                def _(c=c, s=s):
                    z_first_copy(s, c).start()

                @pl.when(jnp.logical_not(leaves_chip[c]))
                def _(c=c, s=s):
                    w_copy(qa, wq_s, wq_r, s, 1, c).start()
        for s in range(Z_FIRST):
            w_send(qa, wq_s, wq_r, s, 1)

    def hooked(s, hooks):
        for n, ops in hooks.items():
            @pl.when(s == n)
            def _(ops=ops):
                for op, *args in ops:
                    op(*args)

    def group_done(g):
        weight_term(g)
        mate_copy(g).start()

    forward(HALO, qa0[0], qa0[1], kv0[0], kv0[1], None)
    chosen = (lax.broadcasted_iota(jnp.int32, (16, HD), 0), lax.broadcasted_iota(jnp.int32, (16, HD), 1))
    first = (chosen[0] & 7) * 3 + (chosen[0] >> 3) * 64
    take = ((chosen[1] >= first) & (chosen[1] < first + 3) & ((chosen[0] & 7) < 6)).astype(F32).astype(BF)

    def backward_zero():
        own = dot_nt(take, stat[...].astype(BF))
        backward(
            HALO, kv0[0], kv0[1], qa0[0], qa0[1], own[HALO : HALO + 1, :], own[8 + HALO : 9 + HALO, :]
        )

    group_done(0)
    backward_zero()
    relay_kv(0)
    relay_kv(1)

    def forward_step(s, carry):
        hooked(s, BEFORE_FORWARD)
        w_wait(kv, wk_s, wk_r, s)
        forward(
            s, qa[s, 0, 1, 1], qa[s, 1, 1, 1],
            kv[s, 0].reshape(KEYS, HD), kv[s, 1].reshape(KEYS, HD), bias_row(s, False),
        )
        hooked(s, AFTER_FORWARD)
        return carry

    BEFORE_FORWARD = {
        0: [(relay_kv, 2)],
        2: [(own_qa,)],
        3: [(relay_qa, 0)],
        4: [(relay_qa, 1)],
    }
    AFTER_FORWARD = {
        0: [(relay_kv, 3), (group_done, 1), (add_mate, 0)],
        1: [(relay_kv, 4), (group_done, 2), (add_mate, 1)],
        2: [(group_done, 3), (add_mate, 2), (add_x1, 0)],
        3: [(group_done, 4), (add_mate, 3), (add_x1, 1)],
        4: [(group_done, 5), (add_mate, 4), (add_x1, 2)],
    }
    lax.fori_loop(0, HALO, forward_step, 0)

    sb[1, 1] = stat[...].astype(BF)

    def sy_copy(r):
        return pltpu.make_async_remote_copy(
            src_ref=sb.at[1, 1], dst_ref=sb.at[r, 1], send_sem=sy_s.at[0], recv_sem=sy_r.at[r // 2],
            device_id=at(ha_=ha_up if r == 2 else ha_down), device_id_type=MESH,
        )

    def sw_copy(r, c):
        return pltpu.make_async_remote_copy(
            src_ref=sb.at[r, 1], dst_ref=sb.at[r, c],
            send_sem=sw_s.at[c // 2], recv_sem=sw_r.at[c // 2],
            device_id=at(wa_=wa_right if c == 0 else wa_left), device_id_type=MESH,
        )

    def sw_send(r):
        for c in ANY_COLS:
            @pl.when(sends_to[c])
            def _(c=c):
                sw_copy(r, c).start()

    def relay_stats():
        for r in (0, 2):
            sy_copy(r).wait_recv()
            sw_send(r)

    def wait_stats():
        for c in ANY_COLS:
            @pl.when(gets_from[c])
            def _(c=c):
                pltpu.make_async_copy(sb.at[:, 1], sb.at[:, c], sw_r.at[c // 2]).wait()

    for r in (0, 2):
        sy_copy(r).start()
    sw_send(1)
    relay_corner(3)
    relay_corner(4)
    relay_qa(2)
    add_mate(5)
    add_x1(3)
    add_x2(0)
    relay_qa(3)
    add_x2(1)
    relay_stats()
    add_direct(4)
    relay_qa(4)
    add_x2(2)
    add_x2(3)
    add_direct(5)
    wait_stats()
    trow[...] = dot_nt(take, sb[...].reshape(KEYS, HD))

    def backward_step(s, carry):
        wait_qa(s)
        backward(
            s, kv[s, 0, 1, 1], kv[s, 1, 1, 1], qa[s, 0].reshape(KEYS, HD), qa[s, 1].reshape(KEYS, HD),
            trow[pl.ds(s, 1), :] - bias_row(s, True), trow[pl.ds(s + 8, 1), :],
        )
        hooked(s, AFTER_BACKWARD)
        return carry

    AFTER_BACKWARD = {
        0: [
            (wait_y, 0), (wait_y, 1), (wait_y, 2), (wait_y, 3), (add_y, 0), (add_y, 1), (send_z, 0),
            (wait_direct, 4), (wait_direct, 5), (add_y, 2), (send_z, 1),
        ],
    }
    lax.fori_loop(0, HALO, backward_step, 0)

    def place_outputs():
        for h in range(HEADS):
            cols = slice(h * HD, (h + 1) * HD)
            for n in range(3):
                grads_out[n, :, cols] = head_value(lambda s: res[n, s], h)

    def left(ref, sem):
        pltpu.make_async_copy(ref, ref, sem).wait()

    def wait_sent():
        for buf, y_send, w_sent in ((kv, yk_s, wk_s), (qa, yq_s, wq_s)):
            for r in (0, 2):
                left(buf.at[:, :, r, 1], y_send.at[r // 2])
            for c in ANY_COLS:
                if buf is kv:
                    @pl.when(sends_to[c])
                    def _(c=c):
                        left(kv.at[:, :, :, c], wk_s.at[c // 2])
                    continue

                @pl.when(jnp.logical_not(leaves_chip[c]))
                def _(c=c):
                    left(qa.at[:, :, :, c], wq_s.at[c // 2])

                @pl.when(sends_to[c] & leaves_chip[c])
                def _(c=c):
                    left(qa.at[0:Z_FIRST, :, :, c], wq_s.at[c // 2])
                    left(qa.at[Z_FIRST:HALO, :, 1, c], zq_s.at[0])
        for c in ANY_COLS:
            @pl.when(gets_from[c] & off_chip[c])
            def _(c=c):
                for r in (0, 2):
                    left(qa.at[Z_FIRST:HALO, :, r, c], yc_s.at[r // 2])
        left(sb.at[0, 0:2], sy_s.at[0])
        for c in ANY_COLS:
            @pl.when(sends_to[c])
            def _(c=c):
                left(sb.at[:, c], sw_s.at[c // 2])
        left(rbuf, dd_s.at[0])
        left(x1buf, x1_s.at[0])
        left(x2buf, x2_s.at[0])
        left(ybuf, yy_s.at[0])
        left(yxbuf, yx_s.at[0])

    def flush():
        @pl.when(own_z)
        def _():
            left(zr.at[0:7], zz_s.at[0])

        @pl.when(jnp.logical_not(own_z))
        def _():
            left(zr, zz_s.at[0])

    place_outputs()
    wait_sent()
    add_z()
    flush()


def put_out(grads, gw, gq_out, gk_out, gv_out, gw_out, sem):
    copies = [
        pltpu.make_async_copy(grads.at[n], ref, sem.at[n]) for n, ref in enumerate((gq_out, gk_out, gv_out))
    ]
    copies.append(pltpu.make_async_copy(gw, gw_out, sem.at[3]))
    for copy in copies:
        copy.start()
    for copy in copies:
        copy.wait()


def shards(queries, key_tiles, value_tiles, out_grad, w_out, reaches):
    dma = pltpu.SemaphoreType.DMA
    vm = pltpu.VMEM
    shapes = [
        pltpu.SMEM((HEADS, 6), jnp.int32),
        vm((TILE, HQ), BF), vm((TILE, HQ), BF), vm((TILE, HQ), BF), vm((TILE, D), BF), vm((D, HQ), BF),
        vm((TILE, HQ), BF), vm((D, TILE), BF),
        vm((HALO, 2, 3, 3, TILE, HD), BF), vm((HALO, 2, 3, 3, TILE, HD), BF),
        vm((2, TILE, HD), BF), vm((2, TILE, HD), BF),
        vm((TILE, HD), F32), vm((3, 3, TILE, HD), BF), vm((16, KEYS), F32),
        vm((TILE, KEYS), F32), vm((TILE, KEYS), F32), vm((TILE, KEYS), BF), vm((TILE, KEYS), BF),
        vm((2, TILE, HD), BF), vm((3, HEADS, TILE, HD), BF),
        vm((6, 2, 4, 192, HD), BF), vm((6, 4, 192, HD), BF), vm((6, 4, 192, HD), BF),
        vm((2, 6, 192, HD), BF), vm((DIRECT, 192, HD), BF), vm((DIRECT, 192, HD), BF),
        vm((6, 4, 48, HD), BF), vm((3, 6, 48, HD), BF),
        vm((HEADS - DIRECT, 4, 48, HD), BF), vm((4, HEADS - DIRECT, 48, HD), BF),
        vm((8, 3, 16, HD), BF), vm((8, 3, 16, HD), BF), vm((6, 8, HD), F32),
        dma((6,)),
    ]
    for sends, receives in (
        ((2,), (HALO, 2)), ((2,), (HALO, 2)), ((2,), (HALO, 2)), ((2,), (HALO, 2)), ((1,), (2,)), ((2,), (2,)),
        ((1,), (6,)), ((1,), (6, 2)), ((1,), (DIRECT,)), ((1,), (6,)), ((1,), (2,)), ((2,), (HALO - Z_FIRST, 2)), ((1,), (HEADS - DIRECT,)),
    ):
        shapes += [dma(sends), dma(receives)]
    shapes.append(dma((1,)))
    anywhere = pl.BlockSpec(memory_space=pl.ANY)
    inside = pl.BlockSpec(memory_space=pltpu.VMEM)
    grads, gw = pl.pallas_call(
        kernel,
        out_shape=(pltpu.VMEM((3, TILE, HQ), BF), pltpu.VMEM((6, HQ), F32)),
        in_specs=[anywhere] * 6,
        out_specs=(inside,) * 2,
        scratch_shapes=shapes,
        compiler_params=pltpu.CompilerParams(collective_id=0, has_side_effects=True),
    )(
        reaches,
        queries.reshape(TILE, HQ),
        key_tiles.reshape(TILE, HQ),
        value_tiles.reshape(TILE, HQ),
        out_grad.reshape(TILE, D),
        w_out,
    )
    tile = jax.ShapeDtypeStruct((TILE, HQ), BF)
    gq, gk, gv, gw = pl.pallas_call(
        put_out,
        out_shape=(tile, tile, tile, jax.ShapeDtypeStruct((6, HQ), F32)),
        in_specs=[inside] * 2,
        out_specs=(anywhere,) * 4,
        scratch_shapes=[dma((4,))],
    )(*(pltpu.with_memory_space_constraint(value, pltpu.VMEM) for value in (grads, gw)))
    return gq.reshape(queries.shape), gk.reshape(queries.shape), gv.reshape(queries.shape), gw


def solution(mesh):
    tiles = P("dp", None, "ha", "wa", None, None)
    return jax.shard_map(
        shards,
        mesh=mesh,
        in_specs=(tiles, tiles, tiles, tiles, P(), P()),
        out_specs=(tiles, tiles, tiles, P(("dp", "ha", "wa"), None)),
        check_vma=False,
    )
```

```python
import math

import jax
import jax.numpy as jnp
from jax import lax
from jax.experimental import pallas as pl
from jax.experimental.pallas import tpu as pltpu
from jax.sharding import PartitionSpec as P

MESH = pl.DeviceIdType.MESH
HEADS = 6
HALO = 5
HD = 128
TILE = 144
KEYS = 9 * TILE
HQ = HEADS * HD
D = 1536
SCALE = 1.0 / math.sqrt(HD)
LOG2E = 1.0 / math.log(2.0)
SCALE2 = SCALE * LOG2E
ROWS = 16
FORWARD_UNROLL = 9
BF = jnp.bfloat16
F32 = jnp.float32
ANY_COLS = (0, 2)
DIRECT = 5
Z_FIRST = 3


def dot(a, b):
    return jnp.dot(a, b, preferred_element_type=F32)


def dot_nt(a, b):
    return lax.dot_general(a, b, (((1,), (1,)), ((), ())), preferred_element_type=F32)


def kernel(
    reach_in, q_in, k_in, v_in, og_in, w_in,
    grads_out, gw_out,
    reach, q_v, k_v, v_v, og_v, w_v, a_v, ogt, kv, qa, kv0, qa0, stat, sb, trow,
    s_buf, dp_buf, p_buf, ds_buf, att_buf, res,
    gbuf, rbuf, abuf, x1buf, xs, x2buf, cbuf, ybuf, xbuf, yxbuf, zbuf, zr, gws,
    in_sem, yk_s, yk_r, yq_s, yq_r, wk_s, wk_r, wq_s, wq_r, sy_s, sy_r, sw_s, sw_r,
    dd_s, dd_r, x1_s, x1_r, x2_s, x2_r, yy_s, yy_r, zz_s, zz_r, yc_s, yc_r, yx_s, yx_r, zq_s,
):
    dp = lax.axis_index("dp")
    ha = lax.axis_index("ha")
    wa = lax.axis_index("wa")
    x = lax.rem(dp, 4)
    z_hi = lax.div(dp, 4)
    core = lax.rem(wa, 2)
    z_lo = lax.div(wa, 2)
    zi = z_hi * 4 + z_lo
    mate = wa + 1 - 2 * core
    x_one = x + 1 - 2 * lax.rem(x, 2)
    x_three = 3 - x
    x_far = lax.rem(x + 2, 4)
    x_a = x_one + core * (x_three - x_one)
    x_b = x_three + core * (x_one - x_three)
    has_left = wa > 0
    has_right = wa < 7

    def at(dp_=dp, ha_=ha, wa_=wa):
        return (dp_, ha_, wa_)

    loads = [
        pltpu.make_async_copy(src, dst, in_sem.at[n])
        for n, (src, dst) in enumerate(
            ((k_in, k_v), (v_in, v_v), (q_in, q_v), (og_in, og_v), (w_in, w_v), (reach_in, reach))
        )
    ]
    for n in (5, 0, 1, 3, 4, 2):
        loads[n].start()

    barrier = pltpu.get_barrier_semaphore()

    def greet(device):
        pl.semaphore_signal(barrier, inc=1, device_id=device, device_id_type=MESH)

    for dy in (1, 2, 3):
        greet(at(ha_=lax.rem(ha + dy, 4)))
        greet(at(dp_=z_hi * 4 + x_b, ha_=lax.rem(ha + dy, 4)))
    greet(at(wa_=mate))
    greet(at(dp_=z_hi * 4 + x_one))
    greet(at(dp_=z_hi * 4 + x_three))

    def z_target(shift, other):
        zl = lax.rem(z_lo + shift, 4)
        to_core = 1 - core if other else core
        return at(dp_=core * 4 + x, wa_=zl * 2 + to_core)

    for dz in range(1, 8):
        zt = lax.rem(zi + dz, 8)
        greet(at(dp_=lax.div(zt, 4) * 4 + x, wa_=lax.rem(zt, 4) * 2 + z_hi))
    own_z = z_hi == core
    far_right = (core == 1) & has_right
    far_left = (core == 0) & has_left

    @pl.when(far_right)
    def _():
        greet(at(wa_=wa + 1))

    @pl.when(far_left)
    def _():
        greet(at(wa_=wa - 1))

    def columns(ref, head):
        return ref[:, head * HD : (head + 1) * HD]

    def slot_columns(ref, slot):
        return jnp.where(slot >= zero_head, columns(ref, slot + 1), columns(ref, slot))

    def zero_columns(ref):
        value = columns(ref, 0)
        for h in range(1, HEADS):
            value = jnp.where(zero_head == h, columns(ref, h), value)
        return value

    def head_value(of_slot, h):
        value = jnp.where(zero_head == h, of_slot(HALO), of_slot(min(h, HALO - 1)))
        return jnp.where(zero_head < h, of_slot(h - 1), value) if h else value

    @pl.when(wa == 0)
    def _():
        for buf in (kv, qa):
            def clear(s, carry, buf=buf):
                for kind in range(2):
                    for r in range(3):
                        buf[s, kind, r, 0] = jnp.zeros((TILE, HD), BF)
                return carry
            lax.fori_loop(0, HALO, clear, 0)
        for r in range(3):
            sb[r, 0] = jnp.zeros((TILE, HD), BF)

    @pl.when(wa == 7)
    def _():
        for buf in (kv, qa):
            def clear(s, carry, buf=buf):
                for kind in range(2):
                    for r in range(3):
                        buf[s, kind, r, 2] = jnp.zeros((TILE, HD), BF)
                return carry
            lax.fori_loop(0, HALO, clear, 0)
        for r in range(3):
            sb[r, 2] = jnp.zeros((TILE, HD), BF)

    loads[5].wait()

    zero_head = jnp.int32(0)
    for n in reversed(range(HEADS)):
        total = reach[n, 0]
        for t in range(1, 6):
            total = total + reach[n, t]
        zero_head = jnp.where(total == 0, n, zero_head)

    loads[0].wait()
    loads[1].wait()

    def place_own_kv():
        for s in range(HALO):
            kv[s, 0, 1, 1] = slot_columns(k_v, s)
            kv[s, 1, 1, 1] = slot_columns(v_v, s)
        kv0[0] = zero_columns(k_v)
        kv0[1] = zero_columns(v_v)

    place_own_kv()

    ha_up = lax.rem(ha + 3, 4)
    ha_down = lax.rem(ha + 1, 4)
    wa_right = jnp.minimum(wa + 1, 7)
    wa_left = jnp.maximum(wa - 1, 0)

    def y_copy(buf, send, recv, s, r):
        return pltpu.make_async_remote_copy(
            src_ref=buf.at[s, :, 1, 1], dst_ref=buf.at[s, :, r, 1],
            send_sem=send.at[r // 2], recv_sem=recv.at[s, r // 2],
            device_id=at(ha_=ha_up if r == 2 else ha_down), device_id_type=MESH,
        )

    def w_copy(buf, send, recv, s, r, c):
        return pltpu.make_async_remote_copy(
            src_ref=buf.at[s, :, r, 1], dst_ref=buf.at[s, :, r, c],
            send_sem=send.at[c // 2], recv_sem=recv.at[s, c // 2],
            device_id=at(wa_=wa_right if c == 0 else wa_left), device_id_type=MESH,
        )

    sends_to = {0: has_right, 2: has_left}
    gets_from = {0: has_left, 2: has_right}

    def w_send(buf, send, recv, s, r):
        for c in ANY_COLS:
            @pl.when(sends_to[c])
            def _(c=c):
                w_copy(buf, send, recv, s, r, c).start()

    def relay(buf, y_send, y_recv, w_s, w_r, s):
        for r in (0, 2):
            y_copy(buf, y_send, y_recv, s, r).wait_recv()
            w_send(buf, w_s, w_r, s, r)

    def w_wait(buf, send, recv, s):
        for c in ANY_COLS:
            @pl.when(gets_from[c])
            def _(c=c):
                pltpu.make_async_copy(buf.at[s, :, :, 1], buf.at[s, :, :, c], recv.at[s, c // 2]).wait()

    def relay_kv(s):
        relay(kv, yk_s, yk_r, wk_s, wk_r, s)

    off_chip = {0: core == 0, 2: core == 1}
    leaves_chip = {0: core == 1, 2: core == 0}

    def relay_qa(s):
        if s < Z_FIRST:
            relay(qa, yq_s, yq_r, wq_s, wq_r, s)
            return
        for r in (0, 2):
            y_copy(qa, yq_s, yq_r, s, r).wait_recv()
            for c in ANY_COLS:
                @pl.when(jnp.logical_not(leaves_chip[c]))
                def _(c=c, r=r):
                    w_copy(qa, wq_s, wq_r, s, r, c).start()

    def corner_copy(s, r, c):
        return pltpu.make_async_remote_copy(
            src_ref=qa.at[s, :, 1, c], dst_ref=qa.at[s, :, r, c],
            send_sem=yc_s.at[r // 2], recv_sem=yc_r.at[s - Z_FIRST, r // 2],
            device_id=at(ha_=ha_up if r == 2 else ha_down), device_id_type=MESH,
        )

    def z_first_copy(s, c):
        return pltpu.make_async_remote_copy(
            src_ref=qa.at[s, :, 1, 1], dst_ref=qa.at[s, :, 1, c],
            send_sem=zq_s.at[0], recv_sem=wq_r.at[s, c // 2],
            device_id=at(wa_=wa_right if c == 0 else wa_left), device_id_type=MESH,
        )

    def relay_corner(s):
        for c in ANY_COLS:
            @pl.when(gets_from[c] & off_chip[c])
            def _(c=c):
                w_copy(qa, wq_s, wq_r, s, 1, c).wait_recv()
                for r in (0, 2):
                    corner_copy(s, r, c).start()

    def wait_qa(s):
        @pl.when(s < Z_FIRST)
        def _():
            w_wait(qa, wq_s, wq_r, s)

        @pl.when(s >= Z_FIRST)
        def _():
            for c in ANY_COLS:
                @pl.when(jnp.logical_not(off_chip[c]))
                def _(c=c):
                    pltpu.make_async_copy(qa.at[s, :, :, 1], qa.at[s, :, :, c], wq_r.at[s, c // 2]).wait()

                @pl.when(gets_from[c] & off_chip[c])
                def _(c=c):
                    for r in (0, 2):
                        corner_copy(s, r, c).wait_recv()

    def wait_barrier():
        pl.semaphore_wait(barrier, 17 - 2 * own_z.astype(jnp.int32) + (far_right | far_left).astype(jnp.int32))

    wait_barrier()

    def first_kv(s, carry):
        for r in (0, 2):
            y_copy(kv, yk_s, yk_r, s, r).start()
        w_send(kv, wk_s, wk_r, s, 1)
        return carry

    lax.fori_loop(0, HALO, first_kv, 0)

    def wait_loads():
        loads[2].wait()
        loads[3].wait()
        loads[4].wait()

    def amat():
        a_v[...] = dot(og_v[...], w_v[...]).astype(BF)

    def place_own_qa():
        for s in range(HALO):
            qa[s, 0, 1, 1] = slot_columns(q_v, s)
            qa[s, 1, 1, 1] = slot_columns(a_v, s)
            for r in (0, 2):
                y_copy(qa, yq_s, yq_r, s, r).start()
        qa0[0] = zero_columns(q_v)
        qa0[1] = zero_columns(a_v)

    eye = (
        lax.broadcasted_iota(jnp.int32, (HD, HD), 0) == lax.broadcasted_iota(jnp.int32, (HD, HD), 1)
    ).astype(F32).astype(BF)

    def transpose_og():
        for t in range(D // HD):
            ogt[t * HD : (t + 1) * HD, :] = dot_nt(eye, og_v[:, t * HD : (t + 1) * HD]).astype(BF)

    wait_loads()
    amat()
    place_own_qa()
    transpose_og()

    stat[...] = jnp.zeros((TILE, HD), F32)
    lane = lax.broadcasted_iota(jnp.int32, (ROWS, HD), 1)
    key_id = lax.broadcasted_iota(jnp.int32, (1, KEYS), 1)
    place = jnp.zeros((1, KEYS), jnp.int32)
    for n in range(1, 9):
        place = place + (key_id >= n * TILE).astype(jnp.int32)
    row_id = (key_id >= 3 * TILE).astype(jnp.int32) + (key_id >= 6 * TILE).astype(jnp.int32)
    col_id = place - 3 * row_id

    def bias_row(s, mirrored):
        later = s >= zero_head
        up, down, left, right = (jnp.where(later, reach[s + 1, t], reach[s, t]) for t in range(2, 6))
        if mirrored:
            up, down, left, right = down, up, right, left

        def bias(ok):
            return jnp.where(ok, 0.0, -jnp.inf).astype(F32)

        b_up = bias((up > 0) & (ha > 0))
        b_down = bias((down > 0) & (ha < 3))
        b_left = bias((left > 0) & has_left)
        b_right = bias((right > 0) & has_right)
        zero = jnp.zeros((1, KEYS), F32)
        by_row = jnp.where(row_id == 0, zero + b_up, jnp.where(row_id == 2, zero + b_down, zero))
        by_col = jnp.where(col_id == 0, zero + b_left, jnp.where(col_id == 2, zero + b_right, zero))
        return by_row + by_col

    def split3(value):
        high = value.astype(BF).astype(F32)
        rest = value - high
        mid = rest.astype(BF).astype(F32)
        return high, mid, rest - mid

    def forward(slot, q, a, k, v, bias):
        n = k.shape[0]
        s_buf[:, :n] = dot_nt(q, k)
        dp_buf[:, :n] = dot_nt(a, v)

        def rows_step(i, carry):
            rows = pl.ds(pl.multiple_of(i * ROWS, ROWS), ROWS)
            s = s_buf[rows, :n] * SCALE2
            if bias is not None:
                s = s + bias
            d = dp_buf[rows, :n]
            peak = jnp.max(s, axis=1, keepdims=True)
            e = jnp.exp2(s - peak)
            total = jnp.sum(e, axis=1, keepdims=True)
            p = e * (1.0 / total)
            delta = jnp.sum(p * d, axis=1, keepdims=True)
            p_buf[rows, :n] = p.astype(BF)
            ds_buf[rows, :n] = (p * (d - delta)).astype(BF)
            block = stat[rows, :]
            for base, parts in ((0, split3(peak + jnp.log(total) * LOG2E)), (64, split3(delta))):
                for t, part in enumerate(parts):
                    block = jnp.where(lane == base + 3 * slot + t, part, block)
            stat[rows, :] = block
            return carry

        lax.fori_loop(0, TILE // ROWS, rows_step, 0, unroll=FORWARD_UNROLL if n == KEYS else True)
        att_buf[lax.rem(slot + 1, 2)] = dot(p_buf[:, :n], v).astype(BF)
        res[0, slot] = (dot(ds_buf[:, :n], k) * SCALE).astype(BF)

    def backward(slot, k, v, q, a, lse_row, delta_row):
        n = q.shape[0]
        s_buf[:, :n] = dot_nt(k, q)
        dp_buf[:, :n] = dot_nt(v, a)

        def rows_step(i, carry):
            rows = pl.ds(pl.multiple_of(i * ROWS, ROWS), ROWS)
            p = jnp.exp2(s_buf[rows, :n] * SCALE2 - lse_row)
            p_buf[rows, :n] = p.astype(BF)
            ds_buf[rows, :n] = (p * (dp_buf[rows, :n] - delta_row)).astype(BF)
            return carry

        lax.fori_loop(0, TILE // ROWS, rows_step, 0)
        res[2, slot] = dot(p_buf[:, :n], a).astype(BF)
        res[1, slot] = (dot(ds_buf[:, :n], q) * SCALE).astype(BF)

    GROUPS = tuple((unit, 1) for unit in range(HEADS))

    def units(group):
        return pl.ds(*GROUPS[group])

    def weight_term(group):
        unit, count = GROUPS[group]
        if count == 2:
            attended = jnp.concatenate([att_buf[0], att_buf[1]], axis=1)
        else:
            attended = att_buf[unit % 2]
        for t in range(8):
            both = dot(ogt[t * 192 : (t + 1) * 192, :], attended).astype(BF)
            for n in range(count):
                gbuf[unit + n, t // 4, t % 4] = both[:, n * HD : (n + 1) * HD]

    def mate_copy(g):
        return pltpu.make_async_remote_copy(
            src_ref=gbuf.at[units(g), 1 - core], dst_ref=rbuf.at[units(g)],
            send_sem=dd_s.at[0], recv_sem=dd_r.at[g], device_id=at(wa_=mate), device_id_type=MESH,
        )

    def x1_copy(g, which):
        return pltpu.make_async_remote_copy(
            src_ref=abuf.at[units(g), x_far if which else x_a], dst_ref=x1buf.at[which, units(g)],
            send_sem=x1_s.at[0], recv_sem=x1_r.at[g, which],
            device_id=at(dp_=z_hi * 4 + x_a), device_id_type=MESH,
        )

    def x2_copy(g):
        return pltpu.make_async_remote_copy(
            src_ref=xs.at[units(g)], dst_ref=x2buf.at[units(g)],
            send_sem=x2_s.at[0], recv_sem=x2_r.at[g],
            device_id=at(dp_=z_hi * 4 + x_b), device_id_type=MESH,
        )

    def y_sum_copy(g, dy):
        to = lax.rem(ha + dy, 4)
        return pltpu.make_async_remote_copy(
            src_ref=cbuf.at[units(g), to], dst_ref=ybuf.at[dy - 1, units(g)],
            send_sem=yy_s.at[0], recv_sem=yy_r.at[g],
            device_id=at(ha_=to), device_id_type=MESH,
        )

    def across_copy(u, dy):
        to = lax.rem(ha + dy, 4)
        return pltpu.make_async_remote_copy(
            src_ref=xbuf.at[u - DIRECT, to], dst_ref=yxbuf.at[dy, u - DIRECT],
            send_sem=yx_s.at[0], recv_sem=yx_r.at[u - DIRECT],
            device_id=at(dp_=z_hi * 4 + x_b, ha_=to), device_id_type=MESH,
        )

    Z_GROUPS = ((0, 2), (2, 1))

    def z_sum_copy(n, shift, other):
        target = lax.rem(z_lo + shift, 4) * 2 + (1 - core if other else core)
        return pltpu.make_async_remote_copy(
            src_ref=zbuf.at[target, pl.ds(*Z_GROUPS[n])],
            dst_ref=zr.at[z_hi * 4 + shift, pl.ds(*Z_GROUPS[n])],
            send_sem=zz_s.at[0], recv_sem=zz_r.at[n],
            device_id=z_target(shift, other), device_id_type=MESH,
        )

    def wide(value):
        return value.astype(F32)

    def unit_range(g):
        return range(GROUPS[g][0], GROUPS[g][0] + GROUPS[g][1])

    def add_mate(g):
        mate_copy(g).wait_recv()

        def add(at_x):
            for u in unit_range(g):
                abuf[u, at_x] = (wide(gbuf[u, core, at_x]) + wide(rbuf[u, at_x])).astype(BF)

        add(x_far)
        x1_copy(g, 1).start()
        add(x_a)
        x1_copy(g, 0).start()
        add(x_b)
        add(x)

    def add_x1(g):
        x1_copy(g, 1).wait_recv()
        for u in unit_range(g):
            xs[u] = (wide(abuf[u, x_b]) + wide(x1buf[1, u])).astype(BF)
        x2_copy(g).start()

    def add_x2(g):
        x1_copy(g, 0).wait_recv()
        x2_copy(g).wait_recv()
        for u in unit_range(g):
            total = wide(abuf[u, x]) + wide(x1buf[0, u]) + wide(x2buf[u])
            cbuf[u] = total.astype(BF).reshape(4, 48, HD)
        for dy in (2, 1, 3):
            y_sum_copy(g, dy).start()

    def wait_y(g):
        pltpu.make_async_copy(ybuf.at[:, units(g)], ybuf.at[:, units(g)], yy_r.at[g]).wait()

    def add_direct(u):
        x1_copy(u, 1).wait_recv()
        total = wide(abuf[u, x_b]) + wide(x1buf[1, u])
        xbuf[u - DIRECT] = total.astype(BF).reshape(4, 48, HD)
        for dy in (2, 1, 3, 0):
            across_copy(u, dy).start()
        x1_copy(u, 0).wait_recv()
        total = wide(abuf[u, x]) + wide(x1buf[0, u])
        cbuf[u] = total.astype(BF).reshape(4, 48, HD)
        for dy in (2, 1, 3):
            y_sum_copy(u, dy).start()

    def wait_direct(u):
        wait_y(u)
        pltpu.make_async_copy(yxbuf.at[:, u - DIRECT], yxbuf.at[:, u - DIRECT], yx_r.at[u - DIRECT]).wait()

    pick = (lax.broadcasted_iota(jnp.int32, (128, 96), 0), lax.broadcasted_iota(jnp.int32, (128, 96), 1))
    spread = (
        ((pick[0] & 7) < 6)
        & (pick[1] == ((pick[0] >> 3) & 1) * 48 + (pick[0] >> 4) * 6 + (pick[0] & 7))
    ).astype(F32).astype(BF)

    def add_y(pair):
        halves = []
        for u in (2 * pair, 2 * pair + 1):
            total = wide(cbuf[u, ha])
            for n in range(3):
                total = total + wide(ybuf[n, u])
            if u >= DIRECT:
                for n in range(4):
                    total = total + wide(yxbuf[n, u - DIRECT])
            halves.append(total.astype(BF))
        rows = dot(spread, jnp.concatenate(halves, axis=0))
        zbuf[:, pair] = rows.astype(BF).reshape(8, 16, HD)

    def send_z(n):
        for shift in (2, 1, 3, 0):
            z_sum_copy(n, shift, True).start()
            if shift:
                z_sum_copy(n, shift, False).start()

        @pl.when(jnp.logical_not(own_z))
        def _():
            z_sum_copy(n, 0, False).start()

        @pl.when(own_z)
        def _():
            pairs = range(Z_GROUPS[n][0], Z_GROUPS[n][0] + Z_GROUPS[n][1])
            for pair in pairs:
                zr[zi - z_lo, pair] = zbuf[z_lo * 2 + core, pair]

    def z_bytes(ref, count, n):
        part = ref.at[0:count, pl.ds(*Z_GROUPS[n])]
        return part, part

    def add_z():
        for n in range(2):
            @pl.when(own_z)
            def _(n=n):
                pltpu.make_async_copy(*z_bytes(zr, 7, n), zz_r.at[n]).wait()

            @pl.when(jnp.logical_not(own_z))
            def _(n=n):
                pltpu.make_async_copy(*z_bytes(zr, 8, n), zz_r.at[n]).wait()
        for pair in range(3):
            total = wide(zr[0, pair])
            for n in range(1, 8):
                total = total + wide(zr[n, pair])
            gws[2 * pair] = total[:8]
            gws[2 * pair + 1] = total[8:]
        for h in range(HEADS):
            gw_out[:, h * HD : (h + 1) * HD] = head_value(lambda s: gws[(s + 1) % HEADS, 0:6, :], h)

    def own_qa():
        for s in range(Z_FIRST, HALO):
            for c in ANY_COLS:
                @pl.when(sends_to[c] & leaves_chip[c])
                def _(c=c, s=s):
                    z_first_copy(s, c).start()

                @pl.when(jnp.logical_not(leaves_chip[c]))
                def _(c=c, s=s):
                    w_copy(qa, wq_s, wq_r, s, 1, c).start()
        for s in range(Z_FIRST):
            w_send(qa, wq_s, wq_r, s, 1)

    def hooked(s, hooks):
        for n, ops in hooks.items():
            @pl.when(s == n)
            def _(ops=ops):
                for op, *args in ops:
                    op(*args)

    def group_done(g):
        weight_term(g)
        mate_copy(g).start()

    forward(HALO, qa0[0], qa0[1], kv0[0], kv0[1], None)
    chosen = (lax.broadcasted_iota(jnp.int32, (16, HD), 0), lax.broadcasted_iota(jnp.int32, (16, HD), 1))
    first = (chosen[0] & 7) * 3 + (chosen[0] >> 3) * 64
    take = ((chosen[1] >= first) & (chosen[1] < first + 3) & ((chosen[0] & 7) < 6)).astype(F32).astype(BF)

    def backward_zero():
        own = dot_nt(take, stat[...].astype(BF))
        backward(
            HALO, kv0[0], kv0[1], qa0[0], qa0[1], own[HALO : HALO + 1, :], own[8 + HALO : 9 + HALO, :]
        )

    group_done(0)
    backward_zero()
    relay_kv(0)
    relay_kv(1)

    def forward_step(s, carry):
        hooked(s, BEFORE_FORWARD)
        w_wait(kv, wk_s, wk_r, s)
        forward(
            s, qa[s, 0, 1, 1], qa[s, 1, 1, 1],
            kv[s, 0].reshape(KEYS, HD), kv[s, 1].reshape(KEYS, HD), bias_row(s, False),
        )
        hooked(s, AFTER_FORWARD)
        return carry

    BEFORE_FORWARD = {
        0: [(relay_kv, 2)],
        2: [(own_qa,)],
        3: [(relay_qa, 0)],
        4: [(relay_qa, 1)],
    }
    AFTER_FORWARD = {
        0: [(relay_kv, 3), (group_done, 1), (add_mate, 0)],
        1: [(relay_kv, 4), (group_done, 2), (add_mate, 1)],
        2: [(group_done, 3), (add_mate, 2), (add_x1, 0)],
        3: [(group_done, 4), (add_mate, 3), (add_x1, 1)],
        4: [(group_done, 5), (add_mate, 4), (add_x1, 2)],
    }
    lax.fori_loop(0, HALO, forward_step, 0)

    sb[1, 1] = stat[...].astype(BF)

    def sy_copy(r):
        return pltpu.make_async_remote_copy(
            src_ref=sb.at[1, 1], dst_ref=sb.at[r, 1], send_sem=sy_s.at[0], recv_sem=sy_r.at[r // 2],
            device_id=at(ha_=ha_up if r == 2 else ha_down), device_id_type=MESH,
        )

    def sw_copy(r, c):
        return pltpu.make_async_remote_copy(
            src_ref=sb.at[r, 1], dst_ref=sb.at[r, c],
            send_sem=sw_s.at[c // 2], recv_sem=sw_r.at[c // 2],
            device_id=at(wa_=wa_right if c == 0 else wa_left), device_id_type=MESH,
        )

    def sw_send(r):
        for c in ANY_COLS:
            @pl.when(sends_to[c])
            def _(c=c):
                sw_copy(r, c).start()

    def relay_stats():
        for r in (0, 2):
            sy_copy(r).wait_recv()
            sw_send(r)

    def wait_stats():
        for c in ANY_COLS:
            @pl.when(gets_from[c])
            def _(c=c):
                pltpu.make_async_copy(sb.at[:, 1], sb.at[:, c], sw_r.at[c // 2]).wait()

    for r in (0, 2):
        sy_copy(r).start()
    sw_send(1)
    relay_corner(3)
    relay_corner(4)
    relay_qa(2)
    add_mate(5)
    add_x1(3)
    add_x2(0)
    relay_qa(3)
    add_x2(1)
    relay_stats()
    add_x1(4)
    relay_qa(4)
    add_x2(2)
    add_direct(5)
    add_x2(3)
    add_x2(4)
    wait_stats()
    trow[...] = dot_nt(take, sb[...].reshape(KEYS, HD))

    def backward_step(s, carry):
        wait_qa(s)
        backward(
            s, kv[s, 0, 1, 1], kv[s, 1, 1, 1], qa[s, 0].reshape(KEYS, HD), qa[s, 1].reshape(KEYS, HD),
            trow[pl.ds(s, 1), :] - bias_row(s, True), trow[pl.ds(s + 8, 1), :],
        )
        hooked(s, AFTER_BACKWARD)
        return carry

    AFTER_BACKWARD = {
        0: [
            (wait_y, 0), (wait_y, 1), (wait_y, 2), (wait_y, 3), (add_y, 0), (add_y, 1), (send_z, 0),
            (wait_y, 4), (wait_direct, 5), (add_y, 2), (send_z, 1),
        ],
    }
    lax.fori_loop(0, HALO, backward_step, 0)

    def place_outputs():
        for h in range(HEADS):
            cols = slice(h * HD, (h + 1) * HD)
            for n in range(3):
                grads_out[n, :, cols] = head_value(lambda s: res[n, s], h)

    def left(ref, sem):
        pltpu.make_async_copy(ref, ref, sem).wait()

    def wait_sent():
        for buf, y_send, w_sent in ((kv, yk_s, wk_s), (qa, yq_s, wq_s)):
            for r in (0, 2):
                left(buf.at[:, :, r, 1], y_send.at[r // 2])
            for c in ANY_COLS:
                if buf is kv:
                    @pl.when(sends_to[c])
                    def _(c=c):
                        left(kv.at[:, :, :, c], wk_s.at[c // 2])
                    continue

                @pl.when(jnp.logical_not(leaves_chip[c]))
                def _(c=c):
                    left(qa.at[:, :, :, c], wq_s.at[c // 2])

                @pl.when(sends_to[c] & leaves_chip[c])
                def _(c=c):
                    left(qa.at[0:Z_FIRST, :, :, c], wq_s.at[c // 2])
                    left(qa.at[Z_FIRST:HALO, :, 1, c], zq_s.at[0])
        for c in ANY_COLS:
            @pl.when(gets_from[c] & off_chip[c])
            def _(c=c):
                for r in (0, 2):
                    left(qa.at[Z_FIRST:HALO, :, r, c], yc_s.at[r // 2])
        left(sb.at[0, 0:2], sy_s.at[0])
        for c in ANY_COLS:
            @pl.when(sends_to[c])
            def _(c=c):
                left(sb.at[:, c], sw_s.at[c // 2])
        left(rbuf, dd_s.at[0])
        left(x1buf, x1_s.at[0])
        left(x2buf, x2_s.at[0])
        left(ybuf, yy_s.at[0])
        left(yxbuf, yx_s.at[0])

    def flush():
        @pl.when(own_z)
        def _():
            left(zr.at[0:7], zz_s.at[0])

        @pl.when(jnp.logical_not(own_z))
        def _():
            left(zr, zz_s.at[0])

    place_outputs()
    wait_sent()
    add_z()
    flush()


def put_out(grads, gw, gq_out, gk_out, gv_out, gw_out, sem):
    copies = [
        pltpu.make_async_copy(grads.at[n], ref, sem.at[n]) for n, ref in enumerate((gq_out, gk_out, gv_out))
    ]
    copies.append(pltpu.make_async_copy(gw, gw_out, sem.at[3]))
    for copy in copies:
        copy.start()
    for copy in copies:
        copy.wait()


def shards(queries, key_tiles, value_tiles, out_grad, w_out, reaches):
    dma = pltpu.SemaphoreType.DMA
    vm = pltpu.VMEM
    shapes = [
        pltpu.SMEM((HEADS, 6), jnp.int32),
        vm((TILE, HQ), BF), vm((TILE, HQ), BF), vm((TILE, HQ), BF), vm((TILE, D), BF), vm((D, HQ), BF),
        vm((TILE, HQ), BF), vm((D, TILE), BF),
        vm((HALO, 2, 3, 3, TILE, HD), BF), vm((HALO, 2, 3, 3, TILE, HD), BF),
        vm((2, TILE, HD), BF), vm((2, TILE, HD), BF),
        vm((TILE, HD), F32), vm((3, 3, TILE, HD), BF), vm((16, KEYS), F32),
        vm((TILE, KEYS), F32), vm((TILE, KEYS), F32), vm((TILE, KEYS), BF), vm((TILE, KEYS), BF),
        vm((2, TILE, HD), BF), vm((3, HEADS, TILE, HD), BF),
        vm((6, 2, 4, 192, HD), BF), vm((6, 4, 192, HD), BF), vm((6, 4, 192, HD), BF),
        vm((2, 6, 192, HD), BF), vm((DIRECT, 192, HD), BF), vm((DIRECT, 192, HD), BF),
        vm((6, 4, 48, HD), BF), vm((3, 6, 48, HD), BF),
        vm((HEADS - DIRECT, 4, 48, HD), BF), vm((4, HEADS - DIRECT, 48, HD), BF),
        vm((8, 3, 16, HD), BF), vm((8, 3, 16, HD), BF), vm((6, 8, HD), F32),
        dma((6,)),
    ]
    for sends, receives in (
        ((2,), (HALO, 2)), ((2,), (HALO, 2)), ((2,), (HALO, 2)), ((2,), (HALO, 2)), ((1,), (2,)), ((2,), (2,)),
        ((1,), (6,)), ((1,), (6, 2)), ((1,), (DIRECT,)), ((1,), (6,)), ((1,), (2,)), ((2,), (HALO - Z_FIRST, 2)), ((1,), (HEADS - DIRECT,)),
    ):
        shapes += [dma(sends), dma(receives)]
    shapes.append(dma((1,)))
    anywhere = pl.BlockSpec(memory_space=pl.ANY)
    inside = pl.BlockSpec(memory_space=pltpu.VMEM)
    grads, gw = pl.pallas_call(
        kernel,
        out_shape=(pltpu.VMEM((3, TILE, HQ), BF), pltpu.VMEM((6, HQ), F32)),
        in_specs=[anywhere] * 6,
        out_specs=(inside,) * 2,
        scratch_shapes=shapes,
        compiler_params=pltpu.CompilerParams(collective_id=0, has_side_effects=True),
    )(
        reaches,
        queries.reshape(TILE, HQ),
        key_tiles.reshape(TILE, HQ),
        value_tiles.reshape(TILE, HQ),
        out_grad.reshape(TILE, D),
        w_out,
    )
    tile = jax.ShapeDtypeStruct((TILE, HQ), BF)
    gq, gk, gv, gw = pl.pallas_call(
        put_out,
        out_shape=(tile, tile, tile, jax.ShapeDtypeStruct((6, HQ), F32)),
        in_specs=[inside] * 2,
        out_specs=(anywhere,) * 4,
        scratch_shapes=[dma((4,))],
    )(*(pltpu.with_memory_space_constraint(value, pltpu.VMEM) for value in (grads, gw)))
    return gq.reshape(queries.shape), gk.reshape(queries.shape), gv.reshape(queries.shape), gw


def solution(mesh):
    tiles = P("dp", None, "ha", "wa", None, None)
    return jax.shard_map(
        shards,
        mesh=mesh,
        in_specs=(tiles, tiles, tiles, tiles, P(), P()),
        out_specs=(tiles, tiles, tiles, P(("dp", "ha", "wa"), None)),
        check_vma=False,
    )
```
